512 devices in a mesh: depth: 2 (over core), lat: 256 (over z, y, x).
Axes of the slice: x: 4, y: 8, z: 8, core: 2. Of those that a mesh axis runs over, the one named last changes fastest.
Arguments:
- temp_old: float32 [256, 1024, 512], P('depth', 'lat'), may hold values from -6 to 6
- source: float32 [256, 1024, 512], P('depth', 'lat'), may hold values from -6 to 6
- lat_couple: float32 [256], P('depth'), may hold values from 0.05 to 0.2
- face_couple: float32 [1], replicated, may hold values from 0.5 to 2
- block_inverse: float32 [256, 128], P('depth'), may hold values from -0.3 to 1.4
Outputs:
- temp_new: float32 [256, 1024, 512], P('depth', 'lat')
The draws below stay inside these ranges and needn't reach their ends.
All inputs are finite; a program needn't handle non-finite values.
Results may differ from the reference program's by a relative error of at most 0.0001.
Values sent between devices are 32-bit elements; how exact they have to be, the bound alone decides.
No kernel may reach another device: no remote copies, remote signals or barrier semaphores. Data moves between devices by JAX's collectives and lax.ppermute only.
A program may use at most 64 MiB of HBM per device.

```python
import math
import jax
import jax.numpy as jnp
from jax import lax

CZ = 128
NY = 512
SWEEPS = 6
NZ = 256
NX = 1024
N_DEPTH = 2


def draw_block_inverse(key, part):
    subkeys = jax.random.split(jax.random.fold_in(key, 17), 3)
    row_layer = jnp.arange(NZ) % CZ
    columns = jnp.arange(CZ)
    on_diagonal = (row_layer[:, None] == columns[None, :]).astype(jnp.float32)
    at_first = (columns[None, :] == 0).astype(jnp.float32)
    diagonal_gain = jnp.exp(jax.random.uniform(subkeys[0], (NZ,), jnp.float32, math.log(0.3), math.log(0.6)))
    spread_noise = jnp.clip(jax.random.normal(subkeys[1], (NZ, CZ), jnp.float32), -1.7, 1.7)
    first_weight = jax.random.uniform(subkeys[2], (NZ,), jnp.float32, 0.25, 0.45)
    matrix = on_diagonal * diagonal_gain[:, None] + spread_noise * (0.1 / math.sqrt(CZ)) + at_first * first_weight[:, None]
    return matrix.astype(jnp.float32)


def block_scale(key, shape, shards, low, top_value):
    level = 1.0
    for axis_at, parts in shards:
        steps = jax.random.uniform(jax.random.fold_in(jax.random.fold_in(key, 6), axis_at), (parts,), jnp.float32, low / len(shards), top_value / len(shards))
        level = level * jnp.repeat(jnp.exp(steps), shape[axis_at] // parts).reshape((-1,) + (1,) * (len(shape) - 1 - axis_at))
    return level


def centred(key, dims, scale, limit, cuts=(), held_as=jnp.bfloat16):
    array = jax.random.normal(key, dims, jnp.float32) * scale
    if len(cuts) > 0:
        array = block_scale(key, dims, cuts, -0.22, 0.18) * array
    return jnp.clip(array, min=-limit, max=limit).astype(held_as)


def setup_inputs(seed: int = 0) -> dict:
    keys = jax.random.split(jax.random.key(seed), 6)
    return {
        "temp_old": centred(keys[0], (NZ, NX, NY), 1.0, 6.0, ((0, 2), (1, 256)), jnp.float32),
        "source": centred(keys[1], (NZ, NX, NY), 1.0, 6.0, ((0, 2), (1, 256)), jnp.float32),
        "lat_couple": jnp.clip(jnp.exp(math.log(0.2) - 1.3862944 * jax.random.uniform(keys[2], (NZ,), jnp.float32) ** block_scale(keys[2], (NZ,), ((0, 2),), -0.2, 0.2)), 0.05, 0.2),
        "face_couple": jnp.clip(jnp.exp(jax.random.uniform(keys[3], (N_DEPTH - 1,), jnp.float32, math.log(0.5), math.log(2.0))), 0.5, 2.0),
        "block_inverse": draw_block_inverse(jax.random.fold_in(keys[5], 71), 0),
    }


def lateral_sum(field):
    padded = jnp.pad(field, ((0, 0), (1, 1), (1, 1)))
    return padded[:, 2:, 1:-1] + padded[:, :-2, 1:-1] + padded[:, 1:-1, 2:] + padded[:, 1:-1, :-2]


def reference(temp_old, source, lat_couple, face_couple, block_inverse):
    field = temp_old
    for sweep_index in range(SWEEPS):
        right_side = source + lat_couple[:, None, None] * lateral_sum(field)
        pieces = []
        carry = jnp.zeros(field.shape[1:], jnp.float32)
        for slab_index in range(N_DEPTH):
            slab_rhs = right_side[slab_index * CZ:(slab_index + 1) * CZ]
            if slab_index + 1 < N_DEPTH:
                slab_rhs = slab_rhs.at[CZ - 1].add(face_couple[slab_index] * field[(slab_index + 1) * CZ])
            if slab_index > 0:
                slab_rhs = slab_rhs.at[0].add(face_couple[slab_index - 1] * carry)
            inverse = block_inverse[slab_index * CZ:(slab_index + 1) * CZ]
            solved = jnp.dot(inverse, slab_rhs.reshape(CZ, -1), precision=lax.Precision.HIGHEST,
                             preferred_element_type=jnp.float32).reshape(slab_rhs.shape)
            carry = solved[CZ - 1]
            pieces.append(solved)
        field = jnp.concatenate(pieces, 0)
    return field
```

```python
import functools
import jax
import jax.numpy as jnp
from jax import lax
from jax.experimental import pallas as pl
from jax.experimental.pallas import tpu as pltpu
from jax.sharding import PartitionSpec as P

SWEEPS = 6
LANES = 128
OVERLAP = 16
PAD = 8
VMEM = pl.BlockSpec(memory_space=pltpu.VMEM)
SMEM = pl.BlockSpec(memory_space=pltpu.SMEM)


def pack_body(core_ref, temp_ref, source_ref, inverse_ref, couple_ref, out_ref):
    rows, half = temp_ref.shape[0], temp_ref.shape[2] // 2
    width = half + OVERLAP
    tiles = half // LANES
    core = core_ref[0]
    low = [(t, 0, LANES, t * LANES) for t in range(tiles)] + [(tiles, 0, OVERLAP, half)]
    high = [(tiles - 1, LANES - OVERLAP, OVERLAP, 0)] + [
        (tiles + t, 0, LANES, OVERLAP + t * LANES) for t in range(tiles)
    ]
    for which, pieces in enumerate((low, high)):

        @pl.when(core == which)
        def _():
            for array, ref in enumerate((temp_ref, source_ref)):
                for row in range(rows):
                    base = (array * rows + row) * width
                    for tile, first, count, place in pieces:
                        block = ref[row, :, tile * LANES : (tile + 1) * LANES].T
                        out_ref[base + place : base + place + count, :] = block[first : first + count]

    base = 2 * rows * width
    out_ref[base : base + LANES, :] = inverse_ref[...].T
    out_ref[base + LANES : base + LANES + 8, :] = jnp.broadcast_to(couple_ref[...], (8, LANES))


def pack(core, temp, source, inverse, couple):
    rows, _, columns = temp.shape
    length = 2 * rows * (columns // 2 + OVERLAP) + LANES + 8
    return pl.pallas_call(
        pack_body,
        out_shape=jax.ShapeDtypeStruct((length, LANES), jnp.float32),
        in_specs=[SMEM, VMEM, VMEM, VMEM, VMEM],
        out_specs=VMEM,
        compiler_params=pltpu.CompilerParams(vmem_limit_bytes=8 * 2**20),
        name="pack",
    )(core, temp, source, inverse, couple)


def split(value):
    high = value.astype(jnp.bfloat16)
    return high, (value - high.astype(jnp.float32)).astype(jnp.bfloat16)


def sweeps_body(rows, width, place_ref, face_ref, mine_ref, other_ref,
                far_up, mid_up, near_up, own, near_down, mid_down, far_down,
                field, rhs_source, high_ref, low_ref):
    core, lat, lat_count = place_ref[0], place_ref[1], place_ref[2]
    face = face_ref[0]
    extent = rows + 2 * SWEEPS
    base = 2 * rows * width

    def clear(index, _):
        for buffer in range(2):
            for slab in range(2):
                field[buffer, slab, index] = jnp.zeros(field.shape[3:], jnp.float32)
        return 0

    lax.fori_loop(0, extent + 2, clear, 0)
    for slab, ref in ((core, mine_ref), (1 - core, other_ref)):
        for row in range(rows):
            field[0, slab, SWEEPS + 1 + row, PAD : PAD + width] = ref[row * width : (row + 1) * width]
            rhs_source[slab, row] = ref[(rows + row) * width : (rows + row + 1) * width]

    is_first = core == 0
    pick = lambda start, count, slab: jnp.where(
        is_first == (slab == 0), mine_ref[start : start + count], other_ref[start : start + count]
    )
    first, second = pick(base, LANES, 0), pick(base, LANES, 1)
    couples = [pick(base + LANES, 8, slab)[0:1] for slab in range(2)]
    across = face * first[:, LANES - 1 : LANES] * second[0:1, :]
    for at, block in (((0, 0), first), ((0, 1), across), ((1, 0), None), ((1, 1), second)):
        where = tuple(slice(k * LANES, (k + 1) * LANES) for k in at)
        if block is None:
            high_ref[where] = jnp.zeros((LANES, LANES), jnp.bfloat16)
            low_ref[where] = jnp.zeros((LANES, LANES), jnp.bfloat16)
        else:
            high_ref[where], low_ref[where] = split(block)
    lane = lax.broadcasted_iota(jnp.int32, (1, LANES), 1)
    face_last = jnp.where(lane == LANES - 1, face, 0.0)

    def advance(source_buffer, row, source_row):
        place = row + 1
        grid_row = lat * rows - SWEEPS + row
        inside = ((grid_row >= 0) & (grid_row < lat_count * rows)).astype(jnp.float32)
        sides = []
        for slab in range(2):
            total = (
                field[source_buffer, slab, place - 1, PAD : PAD + width]
                + field[source_buffer, slab, place + 1, PAD : PAD + width]
            ) + (
                field[source_buffer, slab, place, PAD - 1 : PAD - 1 + width]
                + field[source_buffer, slab, place, PAD + 1 : PAD + 1 + width]
            )
            side = total * (couples[slab] * inside)
            if source_row is not None:
                side = side + rhs_source[slab, source_row]
            sides.append(side)
        under = field[source_buffer, 1, place, PAD : PAD + width]
        sides[0] = sides[0] + pltpu.roll(under, LANES - 1, 1) * face_last
        high, low = split(jnp.concatenate(sides, axis=1))
        dot = functools.partial(jnp.dot, preferred_element_type=jnp.float32)
        solved = dot(high, high_ref[...]) + dot(low, high_ref[...]) + dot(high, low_ref[...])
        for slab in range(2):
            field[1 - source_buffer, slab, place, PAD : PAD + width] = solved[:, slab * LANES : (slab + 1) * LANES]

    def sweep(index, _):
        buffer = lax.rem(index, 2)
        reach = index + 1

        def outer(k, _):
            row = jnp.where(k < reach, SWEEPS - reach + k, SWEEPS + rows + k - reach)
            advance(buffer, row, None)
            return 0

        def inner(k, _):
            advance(buffer, SWEEPS + k, k)
            return 0

        lax.fori_loop(0, 2 * reach, outer, 0)
        lax.fori_loop(0, rows, inner, 0)
        return 0

    lax.fori_loop(0, SWEEPS, sweep, 0)
    start = pl.multiple_of(PAD + OVERLAP * core, 8)
    half = width - OVERLAP
    first_row = 1
    for ref in (far_down, mid_down, near_down, own, near_up, mid_up, far_up):
        for k in range(ref.shape[0]):
            for slab in range(2):
                ref[k, slab] = field[SWEEPS % 2, slab, first_row + k, pl.ds(start, half)]
        first_row += ref.shape[0]


def sweeps(place, face, mine, other, rows, half):
    width = half + OVERLAP
    extent = rows + 2 * SWEEPS
    third = SWEEPS // 3
    shape = lambda count: jax.ShapeDtypeStruct((count, 2, half, LANES), jnp.float32)
    return pl.pallas_call(
        functools.partial(sweeps_body, rows, width),
        out_shape=[shape(k) for k in (third, third, third, rows, third, third, third)],
        in_specs=[SMEM, SMEM, VMEM, VMEM],
        out_specs=[VMEM] * 7,
        scratch_shapes=[
            pltpu.VMEM((2, 2, extent + 2, width + 2 * PAD, LANES), jnp.float32),
            pltpu.VMEM((2, rows, width, LANES), jnp.float32),
            pltpu.VMEM((2 * LANES, 2 * LANES), jnp.bfloat16),
            pltpu.VMEM((2 * LANES, 2 * LANES), jnp.bfloat16),
        ],
        compiler_params=pltpu.CompilerParams(vmem_limit_bytes=32 * 2**20),
        name="sweeps",
    )(place, face, mine, other)


def total_of(slab, row, own, from_low, from_high):
    third = from_low[0].shape[0]
    near_low, mid_low = from_low
    near_high, mid_high = from_high
    low = near_low if row < third else mid_low
    high = mid_high if row < third else near_high
    at = row % third
    return own[row, slab] + low[at, slab] + high[at, slab]


def hand_body(core_ref, own, near_low, mid_low, near_high, mid_high, out_ref):
    slab = 1 - core_ref[0]
    for row in range(own.shape[0]):
        out_ref[row] = total_of(slab, row, own, (near_low, mid_low), (near_high, mid_high))


def finish_body(core_ref, own, near_low, mid_low, near_high, mid_high, other_ref, out_ref):
    core = core_ref[0]
    half = own.shape[2]
    for row in range(own.shape[0]):
        mine = total_of(core, row, own, (near_low, mid_low), (near_high, mid_high))
        other = other_ref[row]
        for tile in range(half // LANES):
            cut = slice(tile * LANES, (tile + 1) * LANES)
            mine_t, other_t = mine[cut].T, other[cut].T
            first = jnp.where(core == 0, mine_t, other_t)
            second = jnp.where(core == 0, other_t, mine_t)
            out_ref[row, :, cut] = first
            out_ref[row, :, half + tile * LANES : half + (tile + 1) * LANES] = second


def local(temp_old, source, lat_couple, face_couple, block_inverse):
    _, rows, columns = temp_old.shape
    half = columns // 2
    core, lat = lax.axis_index("depth"), lax.axis_index("lat")
    lat_count = lax.axis_size("lat")
    core_at = core.reshape(1).astype(jnp.int32)
    place = jnp.stack([core, lat, jnp.int32(lat_count)]).astype(jnp.int32)
    forward = [(i, i + 1) for i in range(lat_count - 1)]
    backward = [(target, origin) for origin, target in forward]
    swap = lambda value: lax.ppermute(value, "depth", [(0, 1), (1, 0)])
    rise = lambda value: lax.ppermute(value, "lat", forward)
    sink = lambda value: lax.ppermute(value, "lat", backward)

    temp, src = temp_old.transpose(1, 0, 2), source.transpose(1, 0, 2)
    couple = lat_couple.reshape(1, LANES)
    other = swap(pack(1 - core_at, temp, src, block_inverse, couple))
    mine = pack(core_at, temp, src, block_inverse, couple)
    far_up, mid_up, near_up, own, near_down, mid_down, far_down = sweeps(
        place, face_couple, mine, other, rows, half
    )
    far_low, far_high = rise(far_up), sink(far_down)
    mid_low, mid_high = rise(mid_up), sink(mid_down)
    near_low, near_high = rise(near_up + far_low), sink(near_down + far_high)
    parts = (own, near_low, mid_low, near_high, mid_high)
    params = pltpu.CompilerParams(vmem_limit_bytes=16 * 2**20)
    handed = pl.pallas_call(
        hand_body,
        out_shape=jax.ShapeDtypeStruct((rows, half, LANES), jnp.float32),
        in_specs=[SMEM] + [VMEM] * 5,
        out_specs=VMEM,
        compiler_params=params,
        name="hand",
    )(core_at, *parts)
    result = pl.pallas_call(
        finish_body,
        out_shape=jax.ShapeDtypeStruct((rows, LANES, columns), jnp.float32),
        in_specs=[SMEM] + [VMEM] * 6,
        out_specs=VMEM,
        compiler_params=params,
        name="finish",
    )(core_at, *parts, swap(handed))
    return result.transpose(1, 0, 2)


def solution(mesh):
    return jax.shard_map(
        local,
        mesh=mesh,
        in_specs=(
            P("depth", "lat", None),
            P("depth", "lat", None),
            P("depth"),
            P(),
            P("depth", None),
        ),
        out_specs=P("depth", "lat", None),
        check_vma=False,
    )
```

```python
import functools
import jax
import jax.numpy as jnp
from jax import lax
from jax.experimental import pallas as pl
from jax.experimental.pallas import tpu as pltpu
from jax.sharding import PartitionSpec as P


SWEEPS = 6
LANES = 128
OVERLAP = 16
PAD = 8
GROUP = 4
VMEM = pl.BlockSpec(memory_space=pltpu.VMEM)
SMEM = pl.BlockSpec(memory_space=pltpu.SMEM)


def pack_body(send, core_ref, temp_ref, source_ref, inverse_ref, couple_ref, out_ref):
    rows, half = temp_ref.shape[0], temp_ref.shape[2] // 2
    width = half + OVERLAP
    tiles = half // LANES
    low = [(t, 0, LANES, t * LANES) for t in range(tiles)] + [(tiles, 0, OVERLAP, half)]
    high = [(tiles - 1, LANES - OVERLAP, OVERLAP, 0)] + [
        (tiles + t, 0, LANES, OVERLAP + t * LANES) for t in range(tiles)
    ]
    for slab in range(2):
        turned = (lambda value: pltpu.roll(value, LANES - 1, 1)) if slab == 1 else (lambda value: value)

        @pl.when(core_ref[0] == slab)
        def _():
            for array, ref in enumerate((temp_ref, source_ref)):
                for row in range(rows):
                    base = (array * rows + row) * width
                    for tile, first, count, place in high if (slab == 1) != send else low:
                        block = turned(ref[row, :, tile * LANES : (tile + 1) * LANES].T)
                        out_ref[base + place : base + place + count, :] = block[first : first + count]
            base = 2 * rows * width
            inverse = turned(inverse_ref[...].T)
            if slab == 1:
                inverse = pltpu.roll(inverse, LANES - 1, 0)
            out_ref[base : base + LANES, :] = inverse
            out_ref[base + LANES : base + LANES + 8, :] = turned(jnp.broadcast_to(couple_ref[...], (8, LANES)))


def pack(send, core, temp, source, inverse, couple):
    rows, _, columns = temp.shape
    length = 2 * rows * (columns // 2 + OVERLAP) + LANES + 8
    return pl.pallas_call(
        functools.partial(pack_body, send),
        out_shape=jax.ShapeDtypeStruct((length, LANES), jnp.float32),
        in_specs=[SMEM, VMEM, VMEM, VMEM, VMEM],
        out_specs=VMEM,
        compiler_params=pltpu.CompilerParams(vmem_limit_bytes=8 * 2**20),
        name="pack_send" if send else "pack_own",
    )(core, temp, source, inverse, couple)


def split(value):
    high = value.astype(jnp.bfloat16)
    return high, (value - high.astype(jnp.float32)).astype(jnp.bfloat16)


class Solver:
    def __init__(self, rows, width, place_ref, face_ref, mine_ref, other_ref, weights):
        self.rows, self.width, self.weights = rows, width, weights
        self.core, self.lat, self.lat_count = place_ref[0], place_ref[1], place_ref[2]
        self.odd = lax.rem(self.lat, 2)
        self.payloads = ((self.core, mine_ref), (1 - self.core, other_ref))
        face = face_ref[0]
        base = 2 * rows * width
        first = self.core == 0

        def pick(start, count, slab):
            return jnp.where(first == (slab == 0), mine_ref[start : start + count], other_ref[start : start + count])

        self.couples = [pick(base + LANES, 8, slab)[0:1] for slab in range(2)]
        for slab in range(2):
            high, low = split(pick(base, LANES, slab))
            weights[slab, :LANES, :LANES] = high
            weights[slab, LANES:, :LANES] = high
            weights[slab, :LANES, LANES:] = low
            weights[slab, LANES:, LANES:] = jnp.zeros((LANES, LANES), jnp.bfloat16)
        lane = lax.broadcasted_iota(jnp.int32, (1, LANES), 1)
        self.face_last = jnp.where(lane == LANES - 1, face, 0.0)

    def inside(self, row):
        grid_row = self.lat * self.rows - SWEEPS + row
        return ((grid_row >= 0) & (grid_row < self.lat_count * self.rows)).astype(jnp.float32)

    def apply(self, slab, sides):
        high, low = split(jnp.concatenate(sides, axis=0))
        both = jnp.dot(
            jnp.concatenate([high, low], axis=1), self.weights[slab], preferred_element_type=jnp.float32
        )
        solved = both[:, :LANES] + both[:, LANES:]
        return [solved[k * self.width : (k + 1) * self.width] for k in range(len(sides))]

    def advance(self, rows, sums, unders, extras, store):
        gains = [[couple * self.inside(row) for couple in self.couples] for row in rows]

        def side(k, slab):
            value = sums(k, slab) * gains[k][slab]
            extra = extras(k, slab)
            return value if extra is None else value + extra

        upper = []
        for k in range(len(rows)):
            value, under = side(k, 0), unders(k)
            upper.append(value if under is None else value + under * self.face_last)
        upper = self.apply(0, upper)
        for k, value in enumerate(upper):
            store(k, 0, value)
        lower = self.apply(
            1, [side(k, 1) + upper[k] * self.face_last for k in range(len(rows))]
        )
        for k, value in enumerate(lower):
            store(k, 1, value)


def clear_pads(ref, lead, width):
    zero = jnp.zeros((PAD, LANES), jnp.float32)
    for index in lead:
        ref[(*index, slice(0, PAD))] = zero
        ref[(*index, slice(PAD + width, 2 * PAD + width))] = zero


def strips_body(rows, width, place_ref, face_ref, mine_ref, other_ref, far_first, far_second, strips, weights, last):
    solver = Solver(rows, width, place_ref, face_ref, mine_ref, other_ref, weights)
    middle = slice(PAD, PAD + width)
    clear_pads(strips, [(j, a, s) for j in range(SWEEPS) for a in range(4) for s in range(2)], width)
    for slab, ref in solver.payloads:
        for row in range(rows):
            strips[0, row, slab, middle] = ref[row * width : (row + 1) * width]
    source = lambda row, slab: jnp.where(
        (solver.core == 0) == (slab == 0),
        mine_ref[(rows + row) * width : (rows + row + 1) * width],
        other_ref[(rows + row) * width : (rows + row + 1) * width],
    )
    top = rows - 1
    for reach in range(1, SWEEPS + 1):
        old = functools.partial(lambda at, a, s, cut: strips[at, a, s, cut], reach - 1)

        def sums(k, slab):
            if k in (0, 3):
                return old(0 if k == 0 else top, slab, middle)
            inner, edge = (1, 0) if k == 1 else (top - 1, top)
            return (
                old(inner, slab, middle)
                + old(edge, slab, slice(PAD - 1, PAD - 1 + width))
                + old(edge, slab, slice(PAD + 1, PAD + 1 + width))
            )

        def unders(k):
            return None if k in (0, 3) else old(0 if k == 1 else top, 1, middle)

        def extras(k, slab):
            return source(0 if k == 1 else top, slab) if reach == 1 and k in (1, 2) else None

        def store(k, slab, value):
            if reach < SWEEPS:
                strips[reach, k, slab, middle] = value
            else:
                last[k, slab] = value

        solver.advance(
            [SWEEPS - reach, SWEEPS + 1 - reach, SWEEPS + top - 1 + reach, SWEEPS + top + reach],
            sums, unders, extras, store,
        )
    start = pl.multiple_of(OVERLAP * solver.core, 8)
    half = width - OVERLAP
    odd = solver.odd
    for ref, row in ((far_first, 2 - 2 * odd), (far_second, 2 * odd)):
        for k in range(2):
            for slab in range(2):
                ref[k, slab] = last[row + k, slab, pl.ds(start, half)]


def core_body(rows, width, place_ref, face_ref, mine_ref, other_ref, strips,
              mid_first, mid_second, near_first, near_second, own, field, rhs_source, weights):
    solver = Solver(rows, width, place_ref, face_ref, mine_ref, other_ref, weights)
    middle = slice(PAD, PAD + width)
    half = width - OVERLAP
    clear_pads(field, [(b, s, r) for b in range(2) for s in range(2) for r in range(2, field.shape[2] - 2)], width)
    for slab, ref in solver.payloads:
        for row in range(rows):
            rhs_source[slab, row] = ref[(rows + row) * width : (rows + row + 1) * width]

    def sweep(reach):
        def old(row, slab, cut):
            low, high = SWEEPS + 1 - reach, SWEEPS + rows - 3 + reach
            if row - low in (0, 1):
                return strips[reach - 1, row - low, slab, cut]
            if row - high in (0, 1):
                return strips[reach - 1, 2 + row - high, slab, cut]
            return field[(reach + 1) % 2, slab, row, cut]

        def group(at):
            def sums(k, slab):
                row = at[k]
                return (old(row - 1, slab, middle) + old(row + 1, slab, middle)) + (
                    old(row, slab, slice(PAD - 1, PAD - 1 + width)) + old(row, slab, slice(PAD + 1, PAD + 1 + width))
                )

            def store(k, slab, value):
                field[reach % 2, slab, at[k], middle] = value

            def extras(k, slab):
                return rhs_source[slab, at[k] - SWEEPS] if 0 <= at[k] - SWEEPS < rows else None

            solver.advance(at, sums, lambda k: old(at[k], 1, middle), extras, store)

        todo = list(range(SWEEPS + 2 - reach, SWEEPS + rows - 2 + reach))
        for first in range(0, len(todo), GROUP):
            group(todo[first : first + GROUP])

    for reach in range(1, SWEEPS + 1):
        sweep(reach)
    start = pl.multiple_of(PAD + OVERLAP * solver.core, 8)
    odd, reach = solver.odd, rows + SWEEPS
    for ref, row in (
        (own, SWEEPS),
        (near_first, reach + (4 - reach) * odd),
        (near_second, 4 + (reach - 4) * odd),
        (mid_first, reach + 2 - reach * odd),
        (mid_second, 2 + reach * odd),
    ):
        for k in range(ref.shape[0]):
            for slab in range(2):
                ref[k, slab] = field[SWEEPS % 2, slab, row + k, pl.ds(start, half)]


def sweeps(place, face, mine, other, rows, half):
    width = half + OVERLAP
    shape = lambda count: jax.ShapeDtypeStruct((count, 2, half, LANES), jnp.float32)
    weights = pltpu.VMEM((2, 2 * LANES, 2 * LANES), jnp.bfloat16)
    far_first, far_second, strips = pl.pallas_call(
        functools.partial(strips_body, rows, width),
        out_shape=[
            shape(2),
            shape(2),
            jax.ShapeDtypeStruct((SWEEPS, 4, 2, width + 2 * PAD, LANES), jnp.float32),
        ],
        in_specs=[SMEM, SMEM, VMEM, VMEM],
        out_specs=[VMEM] * 3,
        scratch_shapes=[weights, pltpu.VMEM((4, 2, width, LANES), jnp.float32)],
        compiler_params=pltpu.CompilerParams(vmem_limit_bytes=24 * 2**20),
        name="strips",
    )(place, face, mine, other)
    mid_first, mid_second, near_first, near_second, own = pl.pallas_call(
        functools.partial(core_body, rows, width),
        out_shape=[shape(k) for k in (2, 2, 2, 2, rows)],
        in_specs=[SMEM, SMEM, VMEM, VMEM, VMEM],
        out_specs=[VMEM] * 5,
        scratch_shapes=[
            pltpu.VMEM((2, 2, rows + 2 * SWEEPS, width + 2 * PAD, LANES), jnp.float32),
            pltpu.VMEM((2, rows, width, LANES), jnp.float32),
            weights,
        ],
        compiler_params=pltpu.CompilerParams(vmem_limit_bytes=32 * 2**20),
        name="core",
    )(place, face, mine, other, strips)
    return far_first, far_second, mid_first, mid_second, near_first, near_second, own


def join_body(place_ref, near, far, same, cross):
    core = place_ref[0]
    for k in range(near.shape[0]):
        same[k] = near[k, core] + far[k, core]
        cross[k] = near[k, 1 - core] + far[k, 1 - core]


def hand_body(place_ref, own, mid_first, mid_second, kept, handed):
    core, odd = place_ref[0], lax.rem(place_ref[1], 2)
    for piece, pair in ((mid_first, odd), (mid_second, 1 - odd)):
        for k in range(2):
            row = 2 * pair + k
            kept[row] = own[row, core] + piece[k, core]
            handed[row] = own[row, 1 - core] + piece[k, 1 - core]


def finish_body(place_ref, kept, handed, same_first, cross_first, same_second, cross_second, out_ref):
    odd = lax.rem(place_ref[1], 2)
    half = kept.shape[1]
    for core in range(2):

        @pl.when(place_ref[0] == core)
        def _():
            for same, cross, pair in ((same_second, cross_second, odd), (same_first, cross_first, 1 - odd)):
                for k in range(2):
                    row = 2 * pair + k
                    for side, base, piece in ((core, kept, same), (1 - core, handed, cross)):
                        for tile in range(half // LANES):
                            cut = slice(tile * LANES, (tile + 1) * LANES)
                            value = base[row, cut] + piece[k, cut]
                            if core == 1:
                                value = pltpu.roll(value, 1, 1)
                            at = side * half + tile * LANES
                            out_ref[row, :, at : at + LANES] = value.T


def program(temp_old, source, lat_couple, face_couple, block_inverse):
    _, rows, columns = temp_old.shape
    half = columns // 2
    core, lat = lax.axis_index("depth"), lax.axis_index("lat")
    lat_count = lax.axis_size("lat")
    place = jnp.stack([core, lat, jnp.int32(lat_count)]).astype(jnp.int32)
    params = pltpu.CompilerParams(vmem_limit_bytes=16 * 2**20)
    piece = lambda *shape: jax.ShapeDtypeStruct((*shape, half, LANES), jnp.float32)

    def call(body, outs, *arrays):
        return pl.pallas_call(
            body, out_shape=outs, in_specs=[SMEM] + [VMEM] * len(arrays), out_specs=[VMEM] * len(outs),
            compiler_params=params,
        )(place, *arrays)

    pairs = [
        [(i, i + 1) for i in range(start, lat_count - 1, 2)] + [(i + 1, i) for i in range(start, lat_count - 1, 2)]
        for start in (0, 1)
    ]
    crossed = [
        [(d * lat_count + a, (1 - d) * lat_count + b) for d in range(2) for a, b in group] for group in pairs
    ]

    swap = lambda value: lax.ppermute(value, "depth", [(0, 1), (1, 0)])
    exchange = lambda value, group: lax.ppermute(value, "lat", pairs[group])
    cross = lambda value, group: lax.ppermute(value, ("depth", "lat"), crossed[group])

    temp, src = temp_old.transpose(1, 0, 2), source.transpose(1, 0, 2)
    couple = lat_couple.reshape(1, LANES)
    other = swap(pack(True, place, temp, src, block_inverse, couple))
    mine = pack(False, place, temp, src, block_inverse, couple)
    far_first, far_second, mid_first, mid_second, near_first, near_second, own = sweeps(
        place, face_couple, mine, other, rows, half
    )
    far_first, far_second = exchange(far_first, 0), exchange(far_second, 1)
    mid_first, mid_second = exchange(mid_first, 0), exchange(mid_second, 1)
    joined = [piece(2), piece(2)]
    same_second, cross_second = call(join_body, joined, near_second, far_first)
    same_second, cross_second = exchange(same_second, 1), cross(cross_second, 1)
    same_first, cross_first = call(join_body, joined, near_first, far_second)
    same_first, cross_first = exchange(same_first, 0), cross(cross_first, 0)
    kept, handed = call(hand_body, [piece(rows), piece(rows)], own, mid_first, mid_second)
    (result,) = call(
        finish_body, [jax.ShapeDtypeStruct((rows, LANES, columns), jnp.float32)],
        kept, swap(handed), same_first, cross_first, same_second, cross_second,
    )
    return result.transpose(1, 0, 2)


def solution(mesh):
    return jax.shard_map(
        program,
        mesh=mesh,
        in_specs=(
            P("depth", "lat", None),
            P("depth", "lat", None),
            P("depth"),
            P(),
            P("depth", None),
        ),
        out_specs=P("depth", "lat", None),
        check_vma=False,
    )
```

```python
import functools
import jax
import jax.numpy as jnp
from jax import lax
from jax.experimental import pallas as pl
from jax.experimental.pallas import tpu as pltpu
from jax.sharding import PartitionSpec as P


SWEEPS = 6
LANES = 128
OVERLAP = 16
PAD = 8
GROUP = 4
VMEM = pl.BlockSpec(memory_space=pltpu.VMEM)
SMEM = pl.BlockSpec(memory_space=pltpu.SMEM)


def position():
    return lax.axis_index("depth"), lax.axis_index("lat")


def lines_of(array):
    layers, rows, columns = array.shape
    return array.reshape(layers, rows, columns // LANES, LANES).transpose(0, 2, 1, 3).reshape(-1, LANES)


def array_of(lines, shape):
    layers, rows, columns = shape
    return lines.reshape(layers, columns // LANES, rows, LANES).transpose(0, 2, 1, 3).reshape(shape)


def pack_lines(send, rows, core, ref, array, out_ref):
    step = ref.shape[0] // (LANES + 1)
    tiles = step // rows // 2
    half = tiles * LANES
    width = half + OVERLAP
    low = [(t, 0, LANES, t * LANES) for t in range(tiles)] + [(tiles, 0, OVERLAP, half)]
    high = [(tiles - 1, LANES - OVERLAP, OVERLAP, 0)] + [
        (tiles + t, 0, LANES, OVERLAP + t * LANES) for t in range(tiles)
    ]
    for slab in range(2):

        @pl.when(core == slab)
        def _():
            for row in range(rows):
                base = (array * rows + row) * width
                for tile, first, count, place in high if (slab == 1) != send else low:
                    line = (slab * 2 * tiles + tile) * rows + row
                    block = ref[pl.ds(line, LANES, stride=step), :].T
                    out_ref[base + place : base + place + count, :] = block[first : first + count]


def pack_send_body(rows, temp_hbm, source_hbm, inverse_hbm, couple_hbm,
                   out_ref, temp_ref, source_ref, inverse_ref, couple_ref, sems):
    core, _ = position()
    lines = temp_hbm.shape[0]
    step = lines // LANES
    copies = []

    def copy(origin, target):
        copies.append(pltpu.make_async_copy(origin, target, sems.at[len(copies)]))
        copies[-1].start()
        return copies[-1]

    waits = []
    for hbm, ref in ((temp_hbm, temp_ref), (source_hbm, source_ref)):
        waits.append((
            copy(hbm, ref.at[pl.ds(0, lines)]),
            copy(hbm.at[pl.ds(0, step)], ref.at[pl.ds(lines, step)]),
        ))
    rest = [copy(inverse_hbm, inverse_ref), copy(couple_hbm, couple_ref)]
    for array, ref in enumerate((temp_ref, source_ref)):
        for wait in waits[array]:
            wait.wait()
        pack_lines(True, rows, core, ref, array, out_ref)
    for wait in rest:
        wait.wait()
    base = out_ref.shape[0] - LANES - 8
    for slab in range(2):
        turned = (lambda value: pltpu.roll(value, LANES - 1, 1)) if slab == 1 else (lambda value: value)

        @pl.when(core == slab)
        def _():
            inverse = turned(inverse_ref[...].T)
            if slab == 1:
                inverse = pltpu.roll(inverse, LANES - 1, 0)
            out_ref[base : base + LANES, :] = inverse
            out_ref[base + LANES : base + LANES + 8, :] = turned(jnp.broadcast_to(couple_ref[...], (8, LANES)))


def pack_own_body(rows, temp_ref, source_ref, sent_ref, out_ref):
    core, _ = position()
    for array, ref in enumerate((temp_ref, source_ref)):
        pack_lines(False, rows, core, ref, array, out_ref)
    base = out_ref.shape[0] - LANES - 8
    out_ref[base:, :] = sent_ref[base:, :]


def pack_send(rows, temp, source, inverse, couple):
    columns = temp.shape[0] // rows
    length = 2 * rows * (columns // 2 + OVERLAP) + LANES + 8
    shape = lambda count: jax.ShapeDtypeStruct((count, LANES), jnp.float32)
    lines = shape(temp.shape[0] // LANES * (LANES + 1))
    return pl.pallas_call(
        functools.partial(pack_send_body, rows),
        out_shape=[shape(length), lines, lines],
        in_specs=[pl.BlockSpec(memory_space=pltpu.HBM)] * 4,
        out_specs=[VMEM] * 3,
        scratch_shapes=[
            pltpu.VMEM(inverse.shape, jnp.float32),
            pltpu.VMEM(couple.shape, jnp.float32),
            pltpu.SemaphoreType.DMA((6,)),
        ],
        compiler_params=pltpu.CompilerParams(vmem_limit_bytes=12 * 2**20),
        name="pack_send",
    )(*(pltpu.with_memory_space_constraint(array, pltpu.HBM) for array in (temp, source, inverse, couple)))


def split(value):
    high = value.astype(jnp.bfloat16)
    return high, (value - high.astype(jnp.float32)).astype(jnp.bfloat16)


class Solver:
    def __init__(self, rows, width, lat_count, face_ref, mine_ref, other_ref, weights):
        self.rows, self.width, self.weights, self.lat_count = rows, width, weights, lat_count
        self.core, self.lat = position()
        self.odd = lax.rem(self.lat, 2)
        self.payloads = ((self.core, mine_ref), (1 - self.core, other_ref))
        base = 2 * rows * width
        first = self.core == 0
        face = face_ref[0]

        def pick(start, count, slab):
            return jnp.where(first == (slab == 0), mine_ref[start : start + count], other_ref[start : start + count])

        self.couples = [pick(base + LANES, 8, slab)[0:1] for slab in range(2)]
        for slab in range(2):
            high, low = split(pick(base, LANES, slab))
            weights[slab, :LANES, :LANES] = high
            weights[slab, LANES:, :LANES] = high
            weights[slab, :LANES, LANES:] = low
            weights[slab, LANES:, LANES:] = jnp.zeros((LANES, LANES), jnp.bfloat16)
        lane = lax.broadcasted_iota(jnp.int32, (1, LANES), 1)
        self.face_last = jnp.where(lane == LANES - 1, face, 0.0)

    def inside(self, row):
        grid_row = self.lat * self.rows - SWEEPS + row
        return ((grid_row >= 0) & (grid_row < self.lat_count * self.rows)).astype(jnp.float32)

    def apply(self, slab, sides):
        high, low = split(jnp.concatenate(sides, axis=0))
        both = jnp.dot(
            jnp.concatenate([high, low], axis=1), self.weights[slab], preferred_element_type=jnp.float32
        )
        solved = both[:, :LANES] + both[:, LANES:]
        return [solved[k * self.width : (k + 1) * self.width] for k in range(len(sides))]

    def advance(self, rows, sums, unders, extras, store):
        gains = [[couple * self.inside(row) for couple in self.couples] for row in rows]

        def side(k, slab):
            value = sums(k, slab) * gains[k][slab]
            extra = extras(k, slab)
            return value if extra is None else value + extra

        upper = []
        for k in range(len(rows)):
            value, under = side(k, 0), unders(k)
            upper.append(value if under is None else value + under * self.face_last)
        upper = self.apply(0, upper)
        for k, value in enumerate(upper):
            store(k, 0, value)
        lower = self.apply(
            1, [side(k, 1) + upper[k] * self.face_last for k in range(len(rows))]
        )
        for k, value in enumerate(lower):
            store(k, 1, value)


def clear_pads(ref, lead, width):
    zero = jnp.zeros((PAD, LANES), jnp.float32)
    for index in lead:
        ref[(*index, slice(0, PAD))] = zero
        ref[(*index, slice(PAD + width, 2 * PAD + width))] = zero


def strips_body(rows, width, lat_count, face_ref, mine_ref, other_ref, far_first, far_second, strips, weights, last):
    solver = Solver(rows, width, lat_count, face_ref, mine_ref, other_ref, weights)
    middle = slice(PAD, PAD + width)
    clear_pads(strips, [(j, a, s) for j in range(SWEEPS) for a in range(4) for s in range(2)], width)
    for slab, ref in solver.payloads:
        for row in range(rows):
            strips[0, row, slab, middle] = ref[row * width : (row + 1) * width]
    source = lambda row, slab: jnp.where(
        (solver.core == 0) == (slab == 0),
        mine_ref[(rows + row) * width : (rows + row + 1) * width],
        other_ref[(rows + row) * width : (rows + row + 1) * width],
    )
    top = rows - 1
    for reach in range(1, SWEEPS + 1):
        old = functools.partial(lambda at, a, s, cut: strips[at, a, s, cut], reach - 1)

        def sums(k, slab):
            if k in (0, 3):
                return old(0 if k == 0 else top, slab, middle)
            inner, edge = (1, 0) if k == 1 else (top - 1, top)
            return (
                old(inner, slab, middle)
                + old(edge, slab, slice(PAD - 1, PAD - 1 + width))
                + old(edge, slab, slice(PAD + 1, PAD + 1 + width))
            )

        def unders(k):
            return None if k in (0, 3) else old(0 if k == 1 else top, 1, middle)

        def extras(k, slab):
            return source(0 if k == 1 else top, slab) if reach == 1 and k in (1, 2) else None

        def store(k, slab, value):
            if reach < SWEEPS:
                strips[reach, k, slab, middle] = value
            else:
                last[k, slab] = value

        solver.advance(
            [SWEEPS - reach, SWEEPS + 1 - reach, SWEEPS + top - 1 + reach, SWEEPS + top + reach],
            sums, unders, extras, store,
        )
    start = pl.multiple_of(OVERLAP * solver.core, 8)
    half = width - OVERLAP
    odd = solver.odd
    for ref, row in ((far_first, 2 - 2 * odd), (far_second, 2 * odd)):
        for k in range(2):
            for slab in range(2):
                ref[k, slab] = last[row + k, slab, pl.ds(start, half)]


def core_body(rows, width, lat_count, face_ref, mine_ref, other_ref, strips,
              mid_first, mid_second, near_first, near_second, own, field, rhs_source, weights):
    solver = Solver(rows, width, lat_count, face_ref, mine_ref, other_ref, weights)
    middle = slice(PAD, PAD + width)
    half = width - OVERLAP
    clear_pads(field, [(b, s, r) for b in range(2) for s in range(2) for r in range(2, field.shape[2] - 2)], width)
    for slab, ref in solver.payloads:
        for row in range(rows):
            rhs_source[slab, row] = ref[(rows + row) * width : (rows + row + 1) * width]

    def sweep(reach):
        def old(row, slab, cut):
            low, high = SWEEPS + 1 - reach, SWEEPS + rows - 3 + reach
            if row - low in (0, 1):
                return strips[reach - 1, row - low, slab, cut]
            if row - high in (0, 1):
                return strips[reach - 1, 2 + row - high, slab, cut]
            return field[(reach + 1) % 2, slab, row, cut]

        def group(at):
            def sums(k, slab):
                row = at[k]
                return (old(row - 1, slab, middle) + old(row + 1, slab, middle)) + (
                    old(row, slab, slice(PAD - 1, PAD - 1 + width)) + old(row, slab, slice(PAD + 1, PAD + 1 + width))
                )

            def store(k, slab, value):
                field[reach % 2, slab, at[k], middle] = value

            def extras(k, slab):
                return rhs_source[slab, at[k] - SWEEPS] if 0 <= at[k] - SWEEPS < rows else None

            solver.advance(at, sums, lambda k: old(at[k], 1, middle), extras, store)

        todo = list(range(SWEEPS + 2 - reach, SWEEPS + rows - 2 + reach))
        for first in range(0, len(todo), GROUP):
            group(todo[first : first + GROUP])

    for reach in range(1, SWEEPS + 1):
        sweep(reach)
    start = pl.multiple_of(PAD + OVERLAP * solver.core, 8)
    odd, reach = solver.odd, rows + SWEEPS
    for ref, row in (
        (own, SWEEPS),
        (near_first, reach + (4 - reach) * odd),
        (near_second, 4 + (reach - 4) * odd),
        (mid_first, reach + 2 - reach * odd),
        (mid_second, 2 + reach * odd),
    ):
        for k in range(ref.shape[0]):
            for slab in range(2):
                ref[k, slab] = field[SWEEPS % 2, slab, row + k, pl.ds(start, half)]


def sweeps(face, mine, other, rows, half, lat_count):
    width = half + OVERLAP
    shape = lambda count: jax.ShapeDtypeStruct((count, 2, half, LANES), jnp.float32)
    weights = pltpu.VMEM((2, 2 * LANES, 2 * LANES), jnp.bfloat16)
    far_first, far_second, strips = pl.pallas_call(
        functools.partial(strips_body, rows, width, lat_count),
        out_shape=[
            shape(2),
            shape(2),
            jax.ShapeDtypeStruct((SWEEPS, 4, 2, width + 2 * PAD, LANES), jnp.float32),
        ],
        in_specs=[SMEM] + [VMEM] * 2,
        out_specs=[VMEM] * 3,
        scratch_shapes=[weights, pltpu.VMEM((4, 2, width, LANES), jnp.float32)],
        compiler_params=pltpu.CompilerParams(vmem_limit_bytes=24 * 2**20),
        name="strips",
    )(face, mine, other)
    mid_first, mid_second, near_first, near_second, own = pl.pallas_call(
        functools.partial(core_body, rows, width, lat_count),
        out_shape=[shape(k) for k in (2, 2, 2, 2, rows)],
        in_specs=[SMEM] + [VMEM] * 3,
        out_specs=[VMEM] * 5,
        scratch_shapes=[
            pltpu.VMEM((2, 2, rows + 2 * SWEEPS, width + 2 * PAD, LANES), jnp.float32),
            pltpu.VMEM((2, rows, width, LANES), jnp.float32),
            weights,
        ],
        compiler_params=pltpu.CompilerParams(vmem_limit_bytes=32 * 2**20),
        name="core",
    )(face, mine, other, strips)
    return far_first, far_second, mid_first, mid_second, near_first, near_second, own


def join_body(near, far, same, cross):
    core, _ = position()
    for k in range(near.shape[0]):
        same[k] = near[k, core] + far[k, core]
        cross[k] = near[k, 1 - core] + far[k, 1 - core]


def hand_body(own, mid_first, mid_second, kept, handed):
    core, lat = position()
    odd = lax.rem(lat, 2)
    for piece, pair in ((mid_first, odd), (mid_second, 1 - odd)):
        for k in range(2):
            row = 2 * pair + k
            kept[row] = own[row, core] + piece[k, core]
            handed[row] = own[row, 1 - core] + piece[k, 1 - core]


def finish_body(kept, handed, same_first, cross_first, same_second, cross_second, out_hbm, lines, sems):
    at_core, lat = position()
    rows, half, _ = kept.shape
    tiles = half // LANES
    step = 2 * tiles * rows
    for core in range(2):
        for odd in range(2):

            @pl.when((at_core == core) & (lax.rem(lat, 2) == odd))
            def _():
                copies = []
                for side, base, pieces in (
                    (core, kept, (same_first, same_second)),
                    (1 - core, handed, (cross_first, cross_second)),
                ):
                    for tile in range(tiles):
                        cut = slice(tile * LANES, (tile + 1) * LANES)
                        place = (side * tiles + tile) * rows
                        for row in range(rows):
                            piece = pieces[1] if row // 2 == odd else pieces[0]
                            value = base[row, cut] + piece[row % 2, cut]
                            lines[pl.ds(core * step + place + row, LANES, stride=step), :] = value.T
                        if core == 1:
                            lines[place : place + rows] = lines[LANES * step + place : LANES * step + place + rows]
                        copies.append(
                            pltpu.make_async_copy(
                                lines.reshape(LANES + 1, step, LANES).at[pl.ds(0, LANES), pl.ds(place, rows)],
                                out_hbm.reshape(LANES, step, LANES).at[:, pl.ds(place, rows)],
                                sems.at[side * tiles + tile],
                            )
                        )
                        copies[-1].start()
                for copy in copies:
                    copy.wait()


def program(temp_old, source, lat_couple, face_couple, block_inverse):
    _, rows, columns = temp_old.shape
    half = columns // 2
    lat_count = lax.axis_size("lat")
    params = pltpu.CompilerParams(vmem_limit_bytes=16 * 2**20)
    piece = lambda *shape: jax.ShapeDtypeStruct((*shape, half, LANES), jnp.float32)

    def call(body, outs, *arrays):
        return pl.pallas_call(
            body, out_shape=outs, in_specs=[VMEM] * len(arrays), out_specs=[VMEM] * len(outs),
            compiler_params=params,
        )(*arrays)

    pairs = [
        [(i, i + 1) for i in range(start, lat_count - 1, 2)] + [(i + 1, i) for i in range(start, lat_count - 1, 2)]
        for start in (0, 1)
    ]
    crossed = [
        [(d * lat_count + a, (1 - d) * lat_count + b) for d in range(2) for a, b in group] for group in pairs
    ]

    swap = lambda value: lax.ppermute(value, "depth", [(0, 1), (1, 0)])
    exchange = lambda value, group: lax.ppermute(value, "lat", pairs[group])
    cross = lambda value, group: lax.ppermute(value, ("depth", "lat"), crossed[group])

    temp, src = lines_of(temp_old), lines_of(source)
    sent, temp, src = pack_send(rows, temp, src, block_inverse, lat_couple.reshape(1, LANES))
    other = swap(sent)
    (mine,) = call(
        functools.partial(pack_own_body, rows), [jax.ShapeDtypeStruct(sent.shape, jnp.float32)], temp, src, sent
    )
    far_first, far_second, mid_first, mid_second, near_first, near_second, own = sweeps(
        face_couple, mine, other, rows, half, lat_count
    )
    far_first, far_second = exchange(far_first, 0), exchange(far_second, 1)
    mid_first, mid_second = exchange(mid_first, 0), exchange(mid_second, 1)
    joined = [piece(2), piece(2)]
    same_second, cross_second = call(join_body, joined, near_second, far_first)
    same_second, cross_second = exchange(same_second, 1), cross(cross_second, 1)
    same_first, cross_first = call(join_body, joined, near_first, far_second)
    same_first, cross_first = exchange(same_first, 0), cross(cross_first, 0)
    kept, handed = call(hand_body, [piece(rows), piece(rows)], own, mid_first, mid_second)
    lines = temp_old.size // LANES
    result = pl.pallas_call(
        finish_body,
        out_shape=jax.ShapeDtypeStruct((lines, LANES), jnp.float32),
        in_specs=[VMEM] * 6,
        out_specs=pl.BlockSpec(memory_space=pltpu.HBM),
        scratch_shapes=[
            pltpu.VMEM((lines // LANES * (LANES + 1), LANES), jnp.float32),
            pltpu.SemaphoreType.DMA((columns // LANES,)),
        ],
        compiler_params=params,
        name="finish",
    )(kept, swap(handed), same_first, cross_first, same_second, cross_second)
    return array_of(result, temp_old.shape)


def solution(mesh):
    return jax.shard_map(
        program,
        mesh=mesh,
        in_specs=(
            P("depth", "lat", None),
            P("depth", "lat", None),
            P("depth"),
            P(),
            P("depth", None),
        ),
        out_specs=P("depth", "lat", None),
        check_vma=False,
    )
```

```python
import functools
import jax
import jax.numpy as jnp
from jax import lax
from jax.experimental import pallas as pl
from jax.experimental.pallas import tpu as pltpu
from jax.sharding import PartitionSpec as P


SWEEPS = 6
LANES = 128
OVERLAP = 16
PAD = 8
GROUP = 4
VMEM = pl.BlockSpec(memory_space=pltpu.VMEM)
SMEM = pl.BlockSpec(memory_space=pltpu.SMEM)


def position():
    return lax.axis_index("depth"), lax.axis_index("lat")


def lines_of(array):
    layers, rows, columns = array.shape
    return array.reshape(layers, rows, columns // LANES, LANES).transpose(0, 2, 1, 3).reshape(-1, LANES)


def array_of(lines, shape):
    layers, rows, columns = shape
    return lines.reshape(layers, columns // LANES, rows, LANES).transpose(0, 2, 1, 3).reshape(shape)


def window_pieces(rows, step, upper):
    tiles = step // rows // 2
    half = tiles * LANES
    if not upper:
        return [(t, 0, LANES, t * LANES) for t in range(tiles)] + [(tiles, 0, OVERLAP, half)]
    return [(tiles + t, 0, LANES, OVERLAP + t * LANES) for t in range(tiles)] + [
        (tiles - 1, LANES - OVERLAP, OVERLAP, 0)
    ]


def pack_piece(rows, slab, ref, array, piece, out_ref, scale=None):
    step = ref.shape[0] // (LANES + 1)
    width = step // rows // 2 * LANES + OVERLAP
    tile, first, count, place = piece
    for row in range(rows):
        base = (array * rows + row) * width + place
        block = ref[pl.ds((slab * step) + tile * rows + row, LANES, stride=step), :].T
        block = block[first : first + count]
        out_ref[base : base + count, :] = block if scale is None else block * scale


def pack_send_body(rows, temp_hbm, source_hbm, inverse_hbm, couple_hbm,
                   out_ref, temp_ref, source_ref, inverse_ref, couple_ref, sems):
    at_core, _ = position()
    step = temp_hbm.shape[0] // LANES
    tiles = step // rows
    arrays = ((temp_hbm, temp_ref), (source_hbm, source_ref))

    def tile_copy(array, tile):
        hbm, ref = arrays[array]
        cut = pl.ds(tile * rows, rows)
        return pltpu.make_async_copy(
            hbm.reshape(LANES, step, LANES).at[:, cut],
            ref.reshape(LANES + 1, step, LANES).at[pl.ds(0, LANES), cut],
            sems.at[array * tiles + tile],
        )

    inverse_copy = pltpu.make_async_copy(inverse_hbm, inverse_ref, sems.at[2 * tiles])
    couple_copy = pltpu.make_async_copy(couple_hbm, couple_ref, sems.at[2 * tiles + 1])
    for slab in range(2):
        pieces = window_pieces(rows, step, slab == 0)
        unused = [tile for tile in range(tiles) if tile not in [piece[0] for piece in pieces]]
        turned = (lambda value: pltpu.roll(value, LANES - 1, 1)) if slab == 1 else (lambda value: value)

        @pl.when(at_core == slab)
        def _():
            inverse_copy.start()
            couple_copy.start()
            for array in range(2):
                for piece in pieces:
                    tile_copy(array, piece[0]).start()
            for array in range(2):
                for tile in unused:
                    tile_copy(array, tile).start()

            def arrive(array, tile):
                tile_copy(array, tile).wait()
                if slab == 1:
                    ref = arrays[array][1]
                    ref[LANES * step + tile * rows : LANES * step + (tile + 1) * rows] = ref[
                        tile * rows : (tile + 1) * rows
                    ]

            inverse_copy.wait()
            couple_copy.wait()
            base = out_ref.shape[0] - LANES - 8
            inverse = turned((inverse_ref[...] * couple_ref[...]).T)
            if slab == 1:
                inverse = pltpu.roll(inverse, LANES - 1, 0)
            out_ref[base : base + LANES, :] = inverse
            scale = 1.0 / turned(jnp.broadcast_to(couple_ref[...], (8, LANES)))
            out_ref[base + LANES :, :] = scale
            for array in range(2):
                for piece in pieces:
                    arrive(array, piece[0])
                    pack_piece(
                        rows, slab, arrays[array][1], array, piece, out_ref, scale[0:1] if array == 1 else None
                    )
            for array in range(2):
                for tile in unused:
                    arrive(array, tile)


def pack_own_body(rows, temp_ref, source_ref, sent_ref, out_ref):
    core, _ = position()
    step = temp_ref.shape[0] // (LANES + 1)
    base = out_ref.shape[0] - LANES - 8
    scale = sent_ref[base + LANES : base + LANES + 1, :]
    for slab in range(2):

        @pl.when(core == slab)
        def _():
            for array, ref in enumerate((temp_ref, source_ref)):
                for piece in window_pieces(rows, step, slab == 1):
                    pack_piece(rows, slab, ref, array, piece, out_ref, scale if array == 1 else None)

    out_ref[base:, :] = sent_ref[base:, :]


def pack_send(rows, temp, source, inverse, couple):
    columns = temp.shape[0] // rows
    length = 2 * rows * (columns // 2 + OVERLAP) + LANES + 8
    shape = lambda count: jax.ShapeDtypeStruct((count, LANES), jnp.float32)
    lines = shape(temp.shape[0] // LANES * (LANES + 1))
    return pl.pallas_call(
        functools.partial(pack_send_body, rows),
        out_shape=[shape(length), lines, lines],
        in_specs=[pl.BlockSpec(memory_space=pltpu.HBM)] * 4,
        out_specs=[VMEM] * 3,
        scratch_shapes=[
            pltpu.VMEM(inverse.shape, jnp.float32),
            pltpu.VMEM(couple.shape, jnp.float32),
            pltpu.SemaphoreType.DMA((2 * columns // LANES + 2,)),
        ],
        compiler_params=pltpu.CompilerParams(vmem_limit_bytes=12 * 2**20),
        name="pack_send",
    )(*(pltpu.with_memory_space_constraint(array, pltpu.HBM) for array in (temp, source, inverse, couple)))


def split(value):
    high = value.astype(jnp.bfloat16)
    return high, (value - high.astype(jnp.float32)).astype(jnp.bfloat16)


class Solver:
    def __init__(self, rows, width, lat_count, face_ref, mine_ref, other_ref, weights):
        self.rows, self.width, self.weights, self.lat_count = rows, width, weights, lat_count
        self.core, self.lat = position()
        self.odd = lax.rem(self.lat, 2)
        self.payloads = ((self.core, mine_ref), (1 - self.core, other_ref))
        base = 2 * rows * width
        first = self.core == 0
        face = face_ref[0]

        def pick(start, count, slab):
            return jnp.where(first == (slab == 0), mine_ref[start : start + count], other_ref[start : start + count])

        for slab in range(2):
            high, low = split(pick(base, LANES, slab))
            weights[slab, :LANES, :LANES] = high
            weights[slab, LANES:, :LANES] = high
            weights[slab, :LANES, LANES:] = low
            weights[slab, LANES:, LANES:] = jnp.zeros((LANES, LANES), jnp.bfloat16)
        lane = lax.broadcasted_iota(jnp.int32, (1, LANES), 1)
        self.face_last = [
            jnp.where(lane == LANES - 1, face * pick(base + LANES, 8, slab)[0:1], 0.0) for slab in range(2)
        ]

    def inside(self, row):
        grid_row = self.lat * self.rows - SWEEPS + row
        return ((grid_row >= 0) & (grid_row < self.lat_count * self.rows)).astype(jnp.float32)

    def apply(self, slab, sides):
        high, low = split(jnp.concatenate(sides, axis=0))
        both = jnp.dot(
            jnp.concatenate([high, low], axis=1), self.weights[slab], preferred_element_type=jnp.float32
        )
        solved = both[:, :LANES] + both[:, LANES:]
        return [solved[k * self.width : (k + 1) * self.width] for k in range(len(sides))]

    def advance(self, rows, sums, unders, extras, store):
        def side(k, slab):
            value = sums(k, slab)
            extra = extras(k, slab)
            return value if extra is None else value + extra

        upper = []
        for k in range(len(rows)):
            value, under = side(k, 0), unders(k)
            upper.append(value if under is None else value + under * self.face_last[0])
        upper = self.apply(0, upper)
        for k, value in enumerate(upper):
            store(k, 0, value)
        lower = self.apply(
            1, [side(k, 1) + upper[k] * self.face_last[1] for k in range(len(rows))]
        )
        for k, value in enumerate(lower):
            store(k, 1, value)


def clear_pads(ref, lead, width):
    zero = jnp.zeros((PAD, LANES), jnp.float32)
    for index in lead:
        ref[(*index, slice(0, PAD))] = zero
        ref[(*index, slice(PAD + width, 2 * PAD + width))] = zero


def strips_body(rows, width, lat_count, face_ref, mine_ref, other_ref, far_first, far_second, strips, weights, last):
    solver = Solver(rows, width, lat_count, face_ref, mine_ref, other_ref, weights)
    middle = slice(PAD, PAD + width)
    clear_pads(strips, [(j, a, s) for j in range(SWEEPS) for a in range(4) for s in range(2)], width)
    for slab, ref in solver.payloads:
        for row in range(rows):
            strips[0, row, slab, middle] = ref[row * width : (row + 1) * width]
    source = lambda row, slab: jnp.where(
        (solver.core == 0) == (slab == 0),
        mine_ref[(rows + row) * width : (rows + row + 1) * width],
        other_ref[(rows + row) * width : (rows + row + 1) * width],
    )
    top = rows - 1
    for reach in range(1, SWEEPS + 1):
        old = functools.partial(lambda at, a, s, cut: strips[at, a, s, cut], reach - 1)

        def sums(k, slab):
            if k in (0, 3):
                return old(0 if k == 0 else top, slab, middle)
            inner, edge = (1, 0) if k == 1 else (top - 1, top)
            return (
                old(inner, slab, middle)
                + old(edge, slab, slice(PAD - 1, PAD - 1 + width))
                + old(edge, slab, slice(PAD + 1, PAD + 1 + width))
            )

        def unders(k):
            return None if k in (0, 3) else old(0 if k == 1 else top, 1, middle)

        def extras(k, slab):
            return source(0 if k == 1 else top, slab) if reach == 1 and k in (1, 2) else None

        def store(k, slab, value):
            if reach < SWEEPS:
                strips[reach, k, slab, middle] = value
            else:
                last[k, slab] = value

        solver.advance(
            [SWEEPS - reach, SWEEPS + 1 - reach, SWEEPS + top - 1 + reach, SWEEPS + top + reach],
            sums, unders, extras, store,
        )
    start = pl.multiple_of(OVERLAP * solver.core, 8)
    half = width - OVERLAP
    odd = solver.odd
    for ref, row in ((far_first, 2 - 2 * odd), (far_second, 2 * odd)):
        for k in range(2):
            for slab in range(2):
                ref[k, slab] = last[row + k, slab, pl.ds(start, half)]


def sums_of(solver, old, at):
    rows, width = solver.rows, solver.width
    middle = slice(PAD, PAD + width)

    def beside(row, step, slab):
        value = old(row + step, slab, middle)
        edges = {-1: (SWEEPS - rows, SWEEPS), 1: (SWEEPS + rows - 1, SWEEPS + 2 * rows - 1)}[step]
        return value * solver.inside(row + step) if row in edges else value

    def sums(k, slab):
        row = at[k]
        return (beside(row, -1, slab) + beside(row, 1, slab)) + (
            old(row, slab, slice(PAD - 1, PAD - 1 + width)) + old(row, slab, slice(PAD + 1, PAD + 1 + width))
        )

    return sums


def middle_body(rows, width, lat_count, face_ref, mine_ref, other_ref, strips,
                mid_first, mid_second, inner, source_ref, weights, last):
    solver = Solver(rows, width, lat_count, face_ref, mine_ref, other_ref, weights)
    middle = slice(PAD, PAD + width)
    clear_pads(inner, [(j, a, s) for j in range(SWEEPS - 1) for a in range(4) for s in range(2)], width)
    for slab, ref in solver.payloads:
        for row in range(rows):
            source_ref[slab, row] = ref[(rows + row) * width : (rows + row + 1) * width]

    def sweep(reach):
        low, high = SWEEPS + 2 - reach, SWEEPS + rows - 4 + reach
        at = [low, low + 1] if reach == 1 else [low, low + 1, high, high + 1]

        def old(row, slab, cut):
            for index, first in ((0, low - 1), (2, high + 1)):
                if row - first in (0, 1):
                    return strips[reach - 1, index + row - first, slab, cut]
            for index, first in ((0, low + 1), (2, high - 1)):
                if row - first in (0, 1):
                    return inner[reach - 2, index + row - first, slab, cut]
            raise ValueError(row)

        def store(k, slab, value):
            if reach == SWEEPS:
                last[k, slab] = value
                return
            inner[reach - 1, k, slab, middle] = value
            if reach == 1:
                inner[reach - 1, 2 + k, slab, middle] = value

        def extras(k, slab):
            return source_ref[slab, at[k] - SWEEPS] if 0 <= at[k] - SWEEPS < rows else None

        solver.advance(at, sums_of(solver, old, at), lambda k: old(at[k], 1, middle), extras, store)

    for reach in range(1, SWEEPS + 1):
        sweep(reach)
    start = pl.multiple_of(OVERLAP * solver.core, 8)
    half = width - OVERLAP
    odd = solver.odd
    for ref, row in ((mid_first, 2 - 2 * odd), (mid_second, 2 * odd)):
        for k in range(2):
            for slab in range(2):
                ref[k, slab] = last[row + k, slab, pl.ds(start, half)]


def core_body(rows, width, lat_count, face_ref, mine_ref, other_ref, inner, source_ref,
              near_first, near_second, own, field, weights):
    solver = Solver(rows, width, lat_count, face_ref, mine_ref, other_ref, weights)
    middle = slice(PAD, PAD + width)
    half = width - OVERLAP
    clear_pads(field, [(b, s, r) for b in range(2) for s in range(2) for r in range(field.shape[2])], width)

    def sweep(reach):
        low, high = SWEEPS + 3 - reach, SWEEPS + rows - 5 + reach

        def old(row, slab, cut):
            for index, first in ((0, low), (2, high)):
                if row - first in (0, 1):
                    return inner[reach - 2, index + row - first, slab, cut]
            return field[(reach + 1) % 2, slab, row - 4, cut]

        def group(at):
            def store(k, slab, value):
                field[reach % 2, slab, at[k] - 4, middle] = value

            def extras(k, slab):
                return source_ref[slab, at[k] - SWEEPS] if 0 <= at[k] - SWEEPS < rows else None

            solver.advance(at, sums_of(solver, old, at), lambda k: old(at[k], 1, middle), extras, store)

        todo = list(range(low + 1, high + 1))
        for first in range(0, len(todo), GROUP):
            group(todo[first : first + GROUP])

    for reach in range(3, SWEEPS + 1):
        sweep(reach)
    start = pl.multiple_of(PAD + OVERLAP * solver.core, 8)
    odd = solver.odd
    for ref, row in ((own, 2), (near_first, 6 - 6 * odd), (near_second, 6 * odd)):
        for k in range(ref.shape[0]):
            for slab in range(2):
                ref[k, slab] = field[SWEEPS % 2, slab, row + k, pl.ds(start, half)]


def sweeps(face, mine, other, rows, half, lat_count):
    width = half + OVERLAP
    shape = lambda count: jax.ShapeDtypeStruct((count, 2, half, LANES), jnp.float32)
    weights = pltpu.VMEM((2, 2 * LANES, 2 * LANES), jnp.bfloat16)
    far_first, far_second, strips = pl.pallas_call(
        functools.partial(strips_body, rows, width, lat_count),
        out_shape=[
            shape(2),
            shape(2),
            jax.ShapeDtypeStruct((SWEEPS, 4, 2, width + 2 * PAD, LANES), jnp.float32),
        ],
        in_specs=[SMEM] + [VMEM] * 2,
        out_specs=[VMEM] * 3,
        scratch_shapes=[weights, pltpu.VMEM((4, 2, width, LANES), jnp.float32)],
        compiler_params=pltpu.CompilerParams(vmem_limit_bytes=24 * 2**20),
        name="strips",
    )(face, mine, other)
    mid_first, mid_second, inner, terms = pl.pallas_call(
        functools.partial(middle_body, rows, width, lat_count),
        out_shape=[
            shape(2),
            shape(2),
            jax.ShapeDtypeStruct((SWEEPS - 1, 4, 2, width + 2 * PAD, LANES), jnp.float32),
            jax.ShapeDtypeStruct((2, rows, width, LANES), jnp.float32),
        ],
        in_specs=[SMEM] + [VMEM] * 3,
        out_specs=[VMEM] * 4,
        scratch_shapes=[weights, pltpu.VMEM((4, 2, width, LANES), jnp.float32)],
        compiler_params=pltpu.CompilerParams(vmem_limit_bytes=32 * 2**20),
        name="middle",
    )(face, mine, other, strips)
    near_first, near_second, own = pl.pallas_call(
        functools.partial(core_body, rows, width, lat_count),
        out_shape=[shape(k) for k in (2, 2, rows)],
        in_specs=[SMEM] + [VMEM] * 4,
        out_specs=[VMEM] * 3,
        scratch_shapes=[pltpu.VMEM((2, 2, rows + 4, width + 2 * PAD, LANES), jnp.float32), weights],
        compiler_params=pltpu.CompilerParams(vmem_limit_bytes=32 * 2**20),
        name="core",
    )(face, mine, other, inner, terms)
    return far_first, far_second, mid_first, mid_second, near_first, near_second, own


def join_body(near, far, same, cross):
    core, _ = position()
    for k in range(near.shape[0]):
        same[k] = near[k, core] + far[k, core]
        cross[k] = near[k, 1 - core] + far[k, 1 - core]


def hand_body(own, mid_first, mid_second, kept, handed):
    core, lat = position()
    odd = lax.rem(lat, 2)
    for piece, pair in ((mid_first, odd), (mid_second, 1 - odd)):
        for k in range(2):
            row = 2 * pair + k
            kept[row] = own[row, core] + piece[k, core]
            handed[row] = own[row, 1 - core] + piece[k, 1 - core]


def finish_body(crossed, base, first, second, *refs):
    out_hbm, lines, sems = refs[-3:]
    at_core, lat = position()
    rows, half, _ = base.shape
    tiles = half // LANES
    step = 2 * tiles * rows
    for core in range(2):
        for odd in range(2):

            @pl.when((at_core == core) & (lax.rem(lat, 2) == odd))
            def _():
                side = 1 - core if crossed else core
                copies = []
                for tile in range(tiles):
                    cut = slice(tile * LANES, (tile + 1) * LANES)
                    for row in range(rows):
                        piece = second if row // 2 == odd else first
                        value = base[row, cut] + piece[row % 2, cut]
                        line = core * tiles * rows + tile * rows + row
                        lines[pl.ds(line, LANES, stride=tiles * rows), :] = value.T
                    if core == 1:
                        last = (LANES * tiles + tile) * rows
                        lines[tile * rows : (tile + 1) * rows] = lines[last : last + rows]
                    copies.append(
                        pltpu.make_async_copy(
                            lines.reshape(LANES + 1, tiles * rows, LANES).at[pl.ds(0, LANES), pl.ds(tile * rows, rows)],
                            out_hbm.reshape(LANES, step, LANES).at[:, pl.ds((side * tiles + tile) * rows, rows)],
                            sems.at[tile],
                        )
                    )
                    copies[-1].start()
                for copy in copies:
                    copy.wait()


def finish(base, first, second, lines, before=None):
    _, half, _ = base.shape
    hbm = pl.BlockSpec(memory_space=pltpu.HBM)
    crossed = before is not None
    return pl.pallas_call(
        functools.partial(finish_body, crossed),
        out_shape=jax.ShapeDtypeStruct((lines, LANES), jnp.float32),
        in_specs=[VMEM] * 3 + [hbm] * crossed,
        out_specs=hbm,
        scratch_shapes=[
            pltpu.VMEM((lines // LANES * (LANES + 1) // 2, LANES), jnp.float32),
            pltpu.SemaphoreType.DMA((half // LANES,)),
        ],
        input_output_aliases={3: 0} if crossed else {},
        compiler_params=pltpu.CompilerParams(vmem_limit_bytes=8 * 2**20),
        name="finish_crossed" if crossed else "finish_own",
    )(base, first, second, *([before] if crossed else []))


def program(temp_old, source, lat_couple, face_couple, block_inverse):
    _, rows, columns = temp_old.shape
    half = columns // 2
    lat_count = lax.axis_size("lat")
    params = pltpu.CompilerParams(vmem_limit_bytes=16 * 2**20)
    piece = lambda *shape: jax.ShapeDtypeStruct((*shape, half, LANES), jnp.float32)

    def call(body, outs, *arrays):
        return pl.pallas_call(
            body, out_shape=outs, in_specs=[VMEM] * len(arrays), out_specs=[VMEM] * len(outs),
            compiler_params=params,
        )(*arrays)

    pairs = [
        [(i, i + 1) for i in range(start, lat_count - 1, 2)] + [(i + 1, i) for i in range(start, lat_count - 1, 2)]
        for start in (0, 1)
    ]
    crossed = [
        [(d * lat_count + a, (1 - d) * lat_count + b) for d in range(2) for a, b in group] for group in pairs
    ]

    swap = lambda value: lax.ppermute(value, "depth", [(0, 1), (1, 0)])
    exchange = lambda value, group: lax.ppermute(value, "lat", pairs[group])
    cross = lambda value, group: lax.ppermute(value, ("depth", "lat"), crossed[group])

    temp, src = lines_of(temp_old), lines_of(source)
    sent, temp, src = pack_send(rows, temp, src, block_inverse, lat_couple.reshape(1, LANES))
    other = swap(sent)
    (mine,) = call(
        functools.partial(pack_own_body, rows), [jax.ShapeDtypeStruct(sent.shape, jnp.float32)], temp, src, sent
    )
    far_first, far_second, mid_first, mid_second, near_first, near_second, own = sweeps(
        face_couple, mine, other, rows, half, lat_count
    )
    far_first, far_second = exchange(far_first, 0), exchange(far_second, 1)
    mid_first, mid_second = exchange(mid_first, 0), exchange(mid_second, 1)
    joined = [piece(2), piece(2)]
    same_second, cross_second = call(join_body, joined, near_second, far_first)
    same_second, cross_second = exchange(same_second, 1), cross(cross_second, 1)
    same_first, cross_first = call(join_body, joined, near_first, far_second)
    same_first, cross_first = exchange(same_first, 0), cross(cross_first, 0)
    kept, handed = call(hand_body, [piece(rows), piece(rows)], own, mid_first, mid_second)
    lines = temp_old.size // LANES
    result = finish(kept, same_first, same_second, lines)
    result = finish(swap(handed), cross_first, cross_second, lines, result)
    return array_of(result, temp_old.shape)


def solution(mesh):
    return jax.shard_map(
        program,
        mesh=mesh,
        in_specs=(
            P("depth", "lat", None),
            P("depth", "lat", None),
            P("depth"),
            P(),
            P("depth", None),
        ),
        out_specs=P("depth", "lat", None),
        check_vma=False,
    )
```

```python
import functools
import jax
import jax.numpy as jnp
from jax import lax
from jax.experimental import pallas as pl
from jax.experimental.pallas import tpu as pltpu
from jax.sharding import PartitionSpec as P


SWEEPS = 6
LANES = 128
OVERLAP = 16
PAD = 8
GROUP = 4
FINISH = ((True,), (False,))
VMEM = pl.BlockSpec(memory_space=pltpu.VMEM)
SMEM = pl.BlockSpec(memory_space=pltpu.SMEM)


def position():
    return lax.axis_index("depth"), lax.axis_index("lat")


def lines_of(array):
    layers, rows, columns = array.shape
    return array.reshape(layers, rows, columns // LANES, LANES).transpose(0, 2, 1, 3).reshape(-1, LANES)


def array_of(lines, shape):
    layers, rows, columns = shape
    return lines.reshape(layers, columns // LANES, rows, LANES).transpose(0, 2, 1, 3).reshape(shape)


def window_pieces(rows, step, upper):
    tiles = step // rows // 2
    half = tiles * LANES
    if not upper:
        return [(t, 0, LANES, t * LANES) for t in range(tiles)] + [(tiles, 0, OVERLAP, half)]
    return [(tiles + t, 0, LANES, OVERLAP + t * LANES) for t in range(tiles)] + [
        (tiles - 1, LANES - OVERLAP, OVERLAP, 0)
    ]


def pack_piece(rows, slab, ref, array, piece, out_ref, scale=None):
    step = ref.shape[0] // (LANES + 1)
    width = step // rows // 2 * LANES + OVERLAP
    tile, first, count, place = piece
    for row in range(rows):
        base = (array * rows + row) * width + place
        block = ref[pl.ds((slab * step) + tile * rows + row, LANES, stride=step), :].T
        block = block[first : first + count]
        out_ref[base : base + count, :] = block if scale is None else block * scale


def pack_send_body(rows, temp_hbm, source_hbm, inverse_hbm, couple_hbm,
                   out_ref, temp_ref, source_ref, inverse_ref, couple_ref, sems):
    at_core, _ = position()
    step = temp_hbm.shape[0] // LANES
    tiles = step // rows
    arrays = ((temp_hbm, temp_ref), (source_hbm, source_ref))

    def tile_copy(array, tile):
        hbm, ref = arrays[array]
        cut = pl.ds(tile * rows, rows)
        return pltpu.make_async_copy(
            hbm.reshape(LANES, step, LANES).at[:, cut],
            ref.reshape(LANES + 1, step, LANES).at[pl.ds(0, LANES), cut],
            sems.at[array * tiles + tile],
        )

    inverse_copy = pltpu.make_async_copy(inverse_hbm, inverse_ref, sems.at[2 * tiles])
    couple_copy = pltpu.make_async_copy(couple_hbm, couple_ref, sems.at[2 * tiles + 1])
    for slab in range(2):
        pieces = window_pieces(rows, step, slab == 0)
        unused = [tile for tile in range(tiles) if tile not in [piece[0] for piece in pieces]]
        turned = (lambda value: pltpu.roll(value, LANES - 1, 1)) if slab == 1 else (lambda value: value)

        @pl.when(at_core == slab)
        def _():
            inverse_copy.start()
            couple_copy.start()
            for array in range(2):
                for piece in pieces:
                    tile_copy(array, piece[0]).start()
            for array in range(2):
                for tile in unused:
                    tile_copy(array, tile).start()

            def arrive(array, tile):
                tile_copy(array, tile).wait()
                if slab == 1:
                    ref = arrays[array][1]
                    ref[LANES * step + tile * rows : LANES * step + (tile + 1) * rows] = ref[
                        tile * rows : (tile + 1) * rows
                    ]

            inverse_copy.wait()
            couple_copy.wait()
            base = out_ref.shape[0] - LANES - 8
            inverse = turned((inverse_ref[...] * couple_ref[...]).T)
            if slab == 1:
                inverse = pltpu.roll(inverse, LANES - 1, 0)
            out_ref[base : base + LANES, :] = inverse
            scale = 1.0 / turned(jnp.broadcast_to(couple_ref[...], (8, LANES)))
            out_ref[base + LANES :, :] = scale
            for array in range(2):
                for piece in pieces:
                    arrive(array, piece[0])
                    pack_piece(
                        rows, slab, arrays[array][1], array, piece, out_ref, scale[0:1] if array == 1 else None
                    )
            for array in range(2):
                for tile in unused:
                    arrive(array, tile)


def pack_own_body(rows, temp_ref, source_ref, sent_ref, out_ref):
    core, _ = position()
    step = temp_ref.shape[0] // (LANES + 1)
    base = out_ref.shape[0] - LANES - 8
    scale = sent_ref[base + LANES : base + LANES + 1, :]
    for slab in range(2):

        @pl.when(core == slab)
        def _():
            for array, ref in enumerate((temp_ref, source_ref)):
                for piece in window_pieces(rows, step, slab == 1):
                    pack_piece(rows, slab, ref, array, piece, out_ref, scale if array == 1 else None)

    out_ref[base:, :] = sent_ref[base:, :]


def pack_send(rows, temp, source, inverse, couple):
    columns = temp.shape[0] // rows
    length = 2 * rows * (columns // 2 + OVERLAP) + LANES + 8
    shape = lambda count: jax.ShapeDtypeStruct((count, LANES), jnp.float32)
    lines = shape(temp.shape[0] // LANES * (LANES + 1))
    return pl.pallas_call(
        functools.partial(pack_send_body, rows),
        out_shape=[shape(length), lines, lines],
        in_specs=[pl.BlockSpec(memory_space=pltpu.HBM)] * 4,
        out_specs=[VMEM] * 3,
        scratch_shapes=[
            pltpu.VMEM(inverse.shape, jnp.float32),
            pltpu.VMEM(couple.shape, jnp.float32),
            pltpu.SemaphoreType.DMA((2 * columns // LANES + 2,)),
        ],
        compiler_params=pltpu.CompilerParams(vmem_limit_bytes=12 * 2**20),
        name="pack_send",
    )(*(pltpu.with_memory_space_constraint(array, pltpu.HBM) for array in (temp, source, inverse, couple)))


def split(value):
    high = value.astype(jnp.bfloat16)
    return high, (value - high.astype(jnp.float32)).astype(jnp.bfloat16)


class Solver:
    def __init__(self, rows, width, lat_count, face_ref, mine_ref, other_ref, weights):
        self.rows, self.width, self.weights, self.lat_count = rows, width, weights, lat_count
        self.core, self.lat = position()
        self.odd = lax.rem(self.lat, 2)
        self.payloads = ((self.core, mine_ref), (1 - self.core, other_ref))
        base = 2 * rows * width
        first = self.core == 0
        face = face_ref[0]

        def pick(start, count, slab):
            return jnp.where(first == (slab == 0), mine_ref[start : start + count], other_ref[start : start + count])

        for slab in range(2):
            high, low = split(pick(base, LANES, slab))
            weights[slab, :LANES, :LANES] = high
            weights[slab, LANES:, :LANES] = high
            weights[slab, :LANES, LANES:] = low
            weights[slab, LANES:, LANES:] = jnp.zeros((LANES, LANES), jnp.bfloat16)
        lane = lax.broadcasted_iota(jnp.int32, (1, LANES), 1)
        self.face_last = [
            jnp.where(lane == LANES - 1, face * pick(base + LANES, 8, slab)[0:1], 0.0) for slab in range(2)
        ]

    def inside(self, row):
        grid_row = self.lat * self.rows - SWEEPS + row
        return ((grid_row >= 0) & (grid_row < self.lat_count * self.rows)).astype(jnp.float32)

    def apply(self, slab, sides):
        high, low = split(jnp.concatenate(sides, axis=0))
        both = jnp.dot(
            jnp.concatenate([high, low], axis=1), self.weights[slab], preferred_element_type=jnp.float32
        )
        solved = both[:, :LANES] + both[:, LANES:]
        return [solved[k * self.width : (k + 1) * self.width] for k in range(len(sides))]

    def advance(self, rows, sums, unders, extras, store):
        def side(k, slab):
            value = sums(k, slab)
            extra = extras(k, slab)
            return value if extra is None else value + extra

        upper = []
        for k in range(len(rows)):
            value, under = side(k, 0), unders(k)
            upper.append(value if under is None else value + under * self.face_last[0])
        upper = self.apply(0, upper)
        for k, value in enumerate(upper):
            store(k, 0, value)
        lower = self.apply(
            1, [side(k, 1) + upper[k] * self.face_last[1] for k in range(len(rows))]
        )
        for k, value in enumerate(lower):
            store(k, 1, value)


def clear_pads(ref, lead, width):
    zero = jnp.zeros((PAD, LANES), jnp.float32)
    for index in lead:
        ref[(*index, slice(0, PAD))] = zero
        ref[(*index, slice(PAD + width, 2 * PAD + width))] = zero


def strips_body(rows, width, lat_count, face_ref, mine_ref, other_ref, far_first, far_second, strips, weights, last):
    solver = Solver(rows, width, lat_count, face_ref, mine_ref, other_ref, weights)
    middle = slice(PAD, PAD + width)
    clear_pads(strips, [(j, a, s) for j in range(SWEEPS) for a in range(4) for s in range(2)], width)
    for slab, ref in solver.payloads:
        for row in range(rows):
            strips[0, row, slab, middle] = ref[row * width : (row + 1) * width]
    source = lambda row, slab: jnp.where(
        (solver.core == 0) == (slab == 0),
        mine_ref[(rows + row) * width : (rows + row + 1) * width],
        other_ref[(rows + row) * width : (rows + row + 1) * width],
    )
    top = rows - 1
    for reach in range(1, SWEEPS + 1):
        old = functools.partial(lambda at, a, s, cut: strips[at, a, s, cut], reach - 1)

        def sums(k, slab):
            if k in (0, 3):
                return old(0 if k == 0 else top, slab, middle)
            inner, edge = (1, 0) if k == 1 else (top - 1, top)
            return (
                old(inner, slab, middle)
                + old(edge, slab, slice(PAD - 1, PAD - 1 + width))
                + old(edge, slab, slice(PAD + 1, PAD + 1 + width))
            )

        def unders(k):
            return None if k in (0, 3) else old(0 if k == 1 else top, 1, middle)

        def extras(k, slab):
            return source(0 if k == 1 else top, slab) if reach == 1 and k in (1, 2) else None

        def store(k, slab, value):
            if reach < SWEEPS:
                strips[reach, k, slab, middle] = value
            else:
                last[k, slab] = value

        at = [SWEEPS - reach, SWEEPS + 1 - reach, SWEEPS + top - 1 + reach, SWEEPS + top + reach]
        for group in [(0,), (3,), (1,), (2,)]:
            solver.advance(
                [at[k] for k in group],
                lambda k, slab, group=group: sums(group[k], slab),
                lambda k, group=group: unders(group[k]),
                lambda k, slab, group=group: extras(group[k], slab),
                lambda k, slab, value, group=group: store(group[k], slab, value),
            )
    start = pl.multiple_of(OVERLAP * solver.core, 8)
    half = width - OVERLAP
    odd = solver.odd
    for ref, row in ((far_first, 2 - 2 * odd), (far_second, 2 * odd)):
        for k in range(2):
            for slab in range(2):
                ref[k, slab] = last[row + k, slab, pl.ds(start, half)]


def sums_of(solver, old, at):
    rows, width = solver.rows, solver.width
    middle = slice(PAD, PAD + width)

    def beside(row, step, slab):
        value = old(row + step, slab, middle)
        edges = {-1: (SWEEPS - rows, SWEEPS), 1: (SWEEPS + rows - 1, SWEEPS + 2 * rows - 1)}[step]
        return value * solver.inside(row + step) if row in edges else value

    def sums(k, slab):
        row = at[k]
        return (beside(row, -1, slab) + beside(row, 1, slab)) + (
            old(row, slab, slice(PAD - 1, PAD - 1 + width)) + old(row, slab, slice(PAD + 1, PAD + 1 + width))
        )

    return sums


def middle_body(rows, width, lat_count, face_ref, mine_ref, other_ref, strips,
                mid_first, mid_second, inner, source_ref, weights, last):
    solver = Solver(rows, width, lat_count, face_ref, mine_ref, other_ref, weights)
    middle = slice(PAD, PAD + width)
    clear_pads(inner, [(j, a, s) for j in range(SWEEPS - 1) for a in range(4) for s in range(2)], width)
    for slab, ref in solver.payloads:
        for row in range(rows):
            source_ref[slab, row] = ref[(rows + row) * width : (rows + row + 1) * width]

    def sweep(reach):
        low, high = SWEEPS + 2 - reach, SWEEPS + rows - 4 + reach
        at = [low, low + 1] if reach == 1 else [low, low + 1, high, high + 1]

        def old(row, slab, cut):
            for index, first in ((0, low - 1), (2, high + 1)):
                if row - first in (0, 1):
                    return strips[reach - 1, index + row - first, slab, cut]
            for index, first in ((0, low + 1), (2, high - 1)):
                if row - first in (0, 1):
                    return inner[reach - 2, index + row - first, slab, cut]
            raise ValueError(row)

        def store(k, slab, value):
            if reach == SWEEPS:
                last[k, slab] = value
                return
            inner[reach - 1, k, slab, middle] = value
            if reach == 1:
                inner[reach - 1, 2 + k, slab, middle] = value

        def extras(k, slab):
            return source_ref[slab, at[k] - SWEEPS] if 0 <= at[k] - SWEEPS < rows else None

        solver.advance(at, sums_of(solver, old, at), lambda k: old(at[k], 1, middle), extras, store)

    for reach in range(1, SWEEPS + 1):
        sweep(reach)
    start = pl.multiple_of(OVERLAP * solver.core, 8)
    half = width - OVERLAP
    odd = solver.odd
    for ref, row in ((mid_first, 2 - 2 * odd), (mid_second, 2 * odd)):
        for k in range(2):
            for slab in range(2):
                ref[k, slab] = last[row + k, slab, pl.ds(start, half)]


def core_body(rows, width, lat_count, face_ref, mine_ref, other_ref, inner, source_ref,
              near_first, near_second, own, field, weights):
    solver = Solver(rows, width, lat_count, face_ref, mine_ref, other_ref, weights)
    middle = slice(PAD, PAD + width)
    half = width - OVERLAP
    clear_pads(field, [(b, s, r) for b in range(2) for s in range(2) for r in range(field.shape[2])], width)

    def sweep(reach):
        low, high = SWEEPS + 3 - reach, SWEEPS + rows - 5 + reach

        def old(row, slab, cut):
            for index, first in ((0, low), (2, high)):
                if row - first in (0, 1):
                    return inner[reach - 2, index + row - first, slab, cut]
            return field[(reach + 1) % 2, slab, row - 4, cut]

        def group(at):
            def store(k, slab, value):
                field[reach % 2, slab, at[k] - 4, middle] = value

            def extras(k, slab):
                return source_ref[slab, at[k] - SWEEPS] if 0 <= at[k] - SWEEPS < rows else None

            solver.advance(at, sums_of(solver, old, at), lambda k: old(at[k], 1, middle), extras, store)

        todo = list(range(low + 1, high + 1))
        for first in range(0, len(todo), GROUP):
            group(todo[first : first + GROUP])

    for reach in range(3, SWEEPS + 1):
        sweep(reach)
    start = pl.multiple_of(PAD + OVERLAP * solver.core, 8)
    odd = solver.odd
    for ref, row in ((own, 2), (near_first, 6 - 6 * odd), (near_second, 6 * odd)):
        for k in range(ref.shape[0]):
            for slab in range(2):
                ref[k, slab] = field[SWEEPS % 2, slab, row + k, pl.ds(start, half)]


def sweeps(face, mine, other, rows, half, lat_count):
    width = half + OVERLAP
    shape = lambda count: jax.ShapeDtypeStruct((count, 2, half, LANES), jnp.float32)
    weights = pltpu.VMEM((2, 2 * LANES, 2 * LANES), jnp.bfloat16)
    far_first, far_second, strips = pl.pallas_call(
        functools.partial(strips_body, rows, width, lat_count),
        out_shape=[
            shape(2),
            shape(2),
            jax.ShapeDtypeStruct((SWEEPS, 4, 2, width + 2 * PAD, LANES), jnp.float32),
        ],
        in_specs=[SMEM] + [VMEM] * 2,
        out_specs=[VMEM] * 3,
        scratch_shapes=[weights, pltpu.VMEM((4, 2, width, LANES), jnp.float32)],
        compiler_params=pltpu.CompilerParams(vmem_limit_bytes=24 * 2**20),
        name="strips",
    )(face, mine, other)
    mid_first, mid_second, inner, terms = pl.pallas_call(
        functools.partial(middle_body, rows, width, lat_count),
        out_shape=[
            shape(2),
            shape(2),
            jax.ShapeDtypeStruct((SWEEPS - 1, 4, 2, width + 2 * PAD, LANES), jnp.float32),
            jax.ShapeDtypeStruct((2, rows, width, LANES), jnp.float32),
        ],
        in_specs=[SMEM] + [VMEM] * 3,
        out_specs=[VMEM] * 4,
        scratch_shapes=[weights, pltpu.VMEM((4, 2, width, LANES), jnp.float32)],
        compiler_params=pltpu.CompilerParams(vmem_limit_bytes=32 * 2**20),
        name="middle",
    )(face, mine, other, strips)
    near_first, near_second, own = pl.pallas_call(
        functools.partial(core_body, rows, width, lat_count),
        out_shape=[shape(k) for k in (2, 2, rows)],
        in_specs=[SMEM] + [VMEM] * 4,
        out_specs=[VMEM] * 3,
        scratch_shapes=[pltpu.VMEM((2, 2, rows + 4, width + 2 * PAD, LANES), jnp.float32), weights],
        compiler_params=pltpu.CompilerParams(vmem_limit_bytes=32 * 2**20),
        name="core",
    )(face, mine, other, inner, terms)
    return far_first, far_second, mid_first, mid_second, near_first, near_second, own


def join_body(near, far, same, cross):
    core, _ = position()
    for k in range(near.shape[0]):
        same[k] = near[k, core] + far[k, core]
        cross[k] = near[k, 1 - core] + far[k, 1 - core]


def hand_body(own, mid_first, mid_second, kept, handed):
    core, lat = position()
    odd = lax.rem(lat, 2)
    for piece, pair in ((mid_first, odd), (mid_second, 1 - odd)):
        for k in range(2):
            row = 2 * pair + k
            kept[row] = own[row, core] + piece[k, core]
            handed[row] = own[row, 1 - core] + piece[k, 1 - core]


def finish_body(crossed, parts, base, *refs):
    pieces = dict(zip(parts, refs))
    out_hbm, lines, sems = refs[-3:]
    at_core, lat = position()
    rows, half, _ = base.shape
    tiles = half // LANES
    step = 2 * tiles * rows
    for core in range(2):
        for odd in range(2):

            @pl.when((at_core == core) & (lax.rem(lat, 2) == odd))
            def _():
                side = 1 - core if crossed else core
                copies = []
                for tile in range(tiles):
                    cut = slice(tile * LANES, (tile + 1) * LANES)
                    todo = [row for row in range(rows) if (row // 2 == odd) in parts]
                    for row in todo:
                        value = base[row, cut] + pieces[row // 2 == odd][row % 2, cut]
                        line = core * tiles * rows + tile * rows + row
                        lines[pl.ds(line, LANES, stride=tiles * rows), :] = value.T
                    at, count = tile * rows + todo[0], len(todo)
                    if core == 1:
                        last = LANES * tiles * rows + at
                        lines[at : at + count] = lines[last : last + count]
                    copies.append(
                        pltpu.make_async_copy(
                            lines.reshape(LANES + 1, tiles * rows, LANES).at[pl.ds(0, LANES), pl.ds(at, count)],
                            out_hbm.reshape(LANES, step, LANES).at[:, pl.ds(side * tiles * rows + at, count)],
                            sems.at[tile],
                        )
                    )
                    copies[-1].start()
                for copy in copies:
                    copy.wait()


def finish(base, pieces, lines, before=None):
    _, half, _ = base.shape
    hbm = pl.BlockSpec(memory_space=pltpu.HBM)
    crossed = before is not None
    return pl.pallas_call(
        functools.partial(finish_body, crossed, tuple(pieces)),
        out_shape=jax.ShapeDtypeStruct((lines, LANES), jnp.float32),
        in_specs=[VMEM] * (1 + len(pieces)) + [hbm] * crossed,
        out_specs=hbm,
        scratch_shapes=[
            pltpu.VMEM((lines // LANES * (LANES + 1) // 2, LANES), jnp.float32),
            pltpu.SemaphoreType.DMA((half // LANES,)),
        ],
        input_output_aliases={1 + len(pieces): 0} if crossed else {},
        compiler_params=pltpu.CompilerParams(vmem_limit_bytes=8 * 2**20),
    )(base, *pieces.values(), *([before] if crossed else []))


def program(temp_old, source, lat_couple, face_couple, block_inverse):
    _, rows, columns = temp_old.shape
    half = columns // 2
    lat_count = lax.axis_size("lat")
    params = pltpu.CompilerParams(vmem_limit_bytes=16 * 2**20)
    piece = lambda *shape: jax.ShapeDtypeStruct((*shape, half, LANES), jnp.float32)

    def call(body, outs, *arrays):
        return pl.pallas_call(
            body, out_shape=outs, in_specs=[VMEM] * len(arrays), out_specs=[VMEM] * len(outs),
            compiler_params=params,
        )(*arrays)

    pairs = [
        [(i, i + 1) for i in range(start, lat_count - 1, 2)] + [(i + 1, i) for i in range(start, lat_count - 1, 2)]
        for start in (0, 1)
    ]
    crossed = [
        [(d * lat_count + a, (1 - d) * lat_count + b) for d in range(2) for a, b in group] for group in pairs
    ]

    swap = lambda value: lax.ppermute(value, "depth", [(0, 1), (1, 0)])
    exchange = lambda value, group: lax.ppermute(value, "lat", pairs[group])
    cross = lambda value, group: lax.ppermute(value, ("depth", "lat"), crossed[group])

    temp, src = lines_of(temp_old), lines_of(source)
    sent, temp, src = pack_send(rows, temp, src, block_inverse, lat_couple.reshape(1, LANES))
    other = swap(sent)
    (mine,) = call(
        functools.partial(pack_own_body, rows), [jax.ShapeDtypeStruct(sent.shape, jnp.float32)], temp, src, sent
    )
    far_first, far_second, mid_first, mid_second, near_first, near_second, own = sweeps(
        face_couple, mine, other, rows, half, lat_count
    )
    far_first, far_second = exchange(far_first, 0), exchange(far_second, 1)
    mid_first, mid_second = exchange(mid_first, 0), exchange(mid_second, 1)
    joined = [piece(2), piece(2)]
    same_second, cross_second = call(join_body, joined, near_second, far_first)
    same_second, cross_second = exchange(same_second, 1), cross(cross_second, 1)
    same_first, cross_first = call(join_body, joined, near_first, far_second)
    same_first, cross_first = exchange(same_first, 0), cross(cross_first, 0)
    kept, handed = call(hand_body, [piece(rows), piece(rows)], own, mid_first, mid_second)
    lines = temp_old.size // LANES
    result = finish(kept, {False: same_first, True: same_second}, lines)
    handed = swap(handed)
    for pieces in FINISH:
        crossed = {False: cross_first, True: cross_second}
        result = finish(handed, {part: crossed[part] for part in pieces}, lines, result)
    return array_of(result, temp_old.shape)


def solution(mesh):
    return jax.shard_map(
        program,
        mesh=mesh,
        in_specs=(
            P("depth", "lat", None),
            P("depth", "lat", None),
            P("depth"),
            P(),
            P("depth", None),
        ),
        out_specs=P("depth", "lat", None),
        check_vma=False,
    )
```

```python
import functools
import jax
import jax.numpy as jnp
from jax import lax
from jax.experimental import pallas as pl
from jax.experimental.pallas import tpu as pltpu
from jax.sharding import PartitionSpec as P


SWEEPS = 6
LANES = 128
OVERLAP = 16
PAD = 8
GROUP = 4
FINISH = ((True,), (False,))
VMEM = pl.BlockSpec(memory_space=pltpu.VMEM)
SMEM = pl.BlockSpec(memory_space=pltpu.SMEM)


def position():
    return lax.axis_index("depth"), lax.axis_index("lat")


def lines_of(array):
    layers, rows, columns = array.shape
    return array.reshape(layers, rows, columns // LANES, LANES).transpose(0, 2, 1, 3).reshape(-1, LANES)


def array_of(lines, shape):
    layers, rows, columns = shape
    return lines.reshape(layers, columns // LANES, rows, LANES).transpose(0, 2, 1, 3).reshape(shape)


def window_pieces(rows, step, upper):
    tiles = step // rows // 2
    half = tiles * LANES
    if not upper:
        return [(t, 0, LANES, t * LANES) for t in range(tiles)] + [(tiles, 0, OVERLAP, half)]
    return [(tiles + t, 0, LANES, OVERLAP + t * LANES) for t in range(tiles)] + [
        (tiles - 1, LANES - OVERLAP, OVERLAP, 0)
    ]


def pack_piece(rows, slab, ref, array, piece, out_ref, scale=None):
    step = ref.shape[0] // (LANES + 1)
    width = step // rows // 2 * LANES + OVERLAP
    tile, first, count, place = piece
    for row in range(rows):
        base = (array * rows + row) * width + place
        block = ref[pl.ds((slab * step) + tile * rows + row, LANES, stride=step), :].T
        block = block[first : first + count]
        out_ref[base : base + count, :] = block if scale is None else block * scale


def tile_copy(rows, hbm, ref, tile, sem):
    target = ref.reshape(LANES + 1, ref.shape[0] // (LANES + 1), LANES)
    cut = pl.ds(tile * rows, rows)
    return pltpu.make_async_copy(
        hbm.reshape(LANES, hbm.shape[0] // LANES, LANES).at[:, cut], target.at[pl.ds(0, LANES), cut], sem
    )


def repeat_first(rows, ref, tile):
    last = ref.shape[0] - ref.shape[0] // (LANES + 1) + tile * rows
    ref[last : last + rows] = ref[tile * rows : (tile + 1) * rows]


def pack_send_body(rows, temp_hbm, source_hbm, inverse_hbm, couple_hbm,
                   out_ref, temp_ref, source_ref, inverse_ref, couple_ref, sems):
    at_core, _ = position()
    step = temp_hbm.shape[0] // LANES
    tiles = step // rows
    arrays = ((temp_hbm, temp_ref), (source_hbm, source_ref))

    def array_copy(array, tile):
        return tile_copy(rows, *arrays[array], tile, sems.at[array * tiles + tile])

    inverse_copy = pltpu.make_async_copy(inverse_hbm, inverse_ref, sems.at[2 * tiles])
    couple_copy = pltpu.make_async_copy(couple_hbm, couple_ref, sems.at[2 * tiles + 1])
    for slab in range(2):
        pieces = window_pieces(rows, step, slab == 0)
        turned = (lambda value: pltpu.roll(value, LANES - 1, 1)) if slab == 1 else (lambda value: value)

        @pl.when(at_core == slab)
        def _():
            inverse_copy.start()
            couple_copy.start()
            for array in range(2):
                for piece in pieces:
                    array_copy(array, piece[0]).start()

            def arrive(array, tile):
                array_copy(array, tile).wait()
                if slab == 1:
                    repeat_first(rows, arrays[array][1], tile)

            inverse_copy.wait()
            couple_copy.wait()
            base = out_ref.shape[0] - LANES - 8
            inverse = turned((inverse_ref[...] * couple_ref[...]).T)
            if slab == 1:
                inverse = pltpu.roll(inverse, LANES - 1, 0)
            out_ref[base : base + LANES, :] = inverse
            scale = 1.0 / turned(jnp.broadcast_to(couple_ref[...], (8, LANES)))
            out_ref[base + LANES :, :] = scale
            for array in range(2):
                for piece in pieces:
                    arrive(array, piece[0])
                    pack_piece(
                        rows, slab, arrays[array][1], array, piece, out_ref, scale[0:1] if array == 1 else None
                    )


def pack_own_body(rows, temp_hbm, source_hbm, temp_ref, source_ref, sent_ref, out_ref, more_temp, more_source, sems):
    core, _ = position()
    step = temp_hbm.shape[0] // LANES
    arrays = ((temp_hbm, temp_ref, more_temp), (source_hbm, source_ref, more_source))
    base = out_ref.shape[0] - LANES - 8
    scale = (None, sent_ref[base + LANES : base + LANES + 1, :])
    for slab in range(2):

        @pl.when(core == slab)
        def _():
            held = [piece[0] for piece in window_pieces(rows, step, slab == 0)]
            pieces = window_pieces(rows, step, slab == 1)
            (tile,) = [at for at in range(step // rows) if at not in held]
            copies = [tile_copy(rows, hbm, more, tile, sems.at[at]) for at, (hbm, _, more) in enumerate(arrays)]
            for copy in copies:
                copy.start()
            for array, (_, ref, _) in enumerate(arrays):
                for piece in pieces:
                    if piece[0] != tile:
                        pack_piece(rows, slab, ref, array, piece, out_ref, scale[array])
            for array, (_, _, more) in enumerate(arrays):
                copies[array].wait()
                if slab == 1:
                    repeat_first(rows, more, tile)
                for piece in pieces:
                    if piece[0] == tile:
                        pack_piece(rows, slab, more, array, piece, out_ref, scale[array])

    out_ref[base:, :] = sent_ref[base:, :]


def pack_own(rows, temp, source, temp_held, source_held, sent):
    hbm = pl.BlockSpec(memory_space=pltpu.HBM)
    lines = pltpu.VMEM(temp_held.shape, jnp.float32)
    return pl.pallas_call(
        functools.partial(pack_own_body, rows),
        out_shape=jax.ShapeDtypeStruct(sent.shape, jnp.float32),
        in_specs=[hbm] * 2 + [VMEM] * 3,
        out_specs=VMEM,
        scratch_shapes=[lines, lines, pltpu.SemaphoreType.DMA((2,))],
        compiler_params=pltpu.CompilerParams(vmem_limit_bytes=12 * 2**20),
        name="pack_own",
    )(*(pltpu.with_memory_space_constraint(array, pltpu.HBM) for array in (temp, source)), temp_held, source_held, sent)


def pack_send(rows, temp, source, inverse, couple):
    columns = temp.shape[0] // rows
    length = 2 * rows * (columns // 2 + OVERLAP) + LANES + 8
    shape = lambda count: jax.ShapeDtypeStruct((count, LANES), jnp.float32)
    lines = shape(temp.shape[0] // LANES * (LANES + 1))
    return pl.pallas_call(
        functools.partial(pack_send_body, rows),
        out_shape=[shape(length), lines, lines],
        in_specs=[pl.BlockSpec(memory_space=pltpu.HBM)] * 4,
        out_specs=[VMEM] * 3,
        scratch_shapes=[
            pltpu.VMEM(inverse.shape, jnp.float32),
            pltpu.VMEM(couple.shape, jnp.float32),
            pltpu.SemaphoreType.DMA((2 * columns // LANES + 2,)),
        ],
        compiler_params=pltpu.CompilerParams(vmem_limit_bytes=12 * 2**20),
        name="pack_send",
    )(*(pltpu.with_memory_space_constraint(array, pltpu.HBM) for array in (temp, source, inverse, couple)))


def split(value):
    high = value.astype(jnp.bfloat16)
    return high, (value - high.astype(jnp.float32)).astype(jnp.bfloat16)


class Solver:
    def __init__(self, rows, width, lat_count, face_ref, mine_ref, other_ref, weights):
        self.rows, self.width, self.weights, self.lat_count = rows, width, weights, lat_count
        self.core, self.lat = position()
        self.odd = lax.rem(self.lat, 2)
        self.payloads = ((self.core, mine_ref), (1 - self.core, other_ref))
        base = 2 * rows * width
        first = self.core == 0
        face = face_ref[0]

        def pick(start, count, slab):
            return jnp.where(first == (slab == 0), mine_ref[start : start + count], other_ref[start : start + count])

        for slab in range(2):
            high, low = split(pick(base, LANES, slab))
            weights[slab, :LANES, :LANES] = high
            weights[slab, LANES:, :LANES] = high
            weights[slab, :LANES, LANES:] = low
            weights[slab, LANES:, LANES:] = jnp.zeros((LANES, LANES), jnp.bfloat16)
        lane = lax.broadcasted_iota(jnp.int32, (1, LANES), 1)
        self.face_last = [
            jnp.where(lane == LANES - 1, face * pick(base + LANES, 8, slab)[0:1], 0.0) for slab in range(2)
        ]

    def inside(self, row):
        grid_row = self.lat * self.rows - SWEEPS + row
        return ((grid_row >= 0) & (grid_row < self.lat_count * self.rows)).astype(jnp.float32)

    def apply(self, slab, sides):
        high, low = split(jnp.concatenate(sides, axis=0))
        both = jnp.dot(
            jnp.concatenate([high, low], axis=1), self.weights[slab], preferred_element_type=jnp.float32
        )
        solved = both[:, :LANES] + both[:, LANES:]
        return [solved[k * self.width : (k + 1) * self.width] for k in range(len(sides))]

    def advance(self, rows, sums, unders, extras, store):
        def side(k, slab):
            value = sums(k, slab)
            extra = extras(k, slab)
            return value if extra is None else value + extra

        upper = []
        for k in range(len(rows)):
            value, under = side(k, 0), unders(k)
            upper.append(value if under is None else value + under * self.face_last[0])
        upper = self.apply(0, upper)
        for k, value in enumerate(upper):
            store(k, 0, value)
        lower = self.apply(
            1, [side(k, 1) + upper[k] * self.face_last[1] for k in range(len(rows))]
        )
        for k, value in enumerate(lower):
            store(k, 1, value)


def clear_pads(ref, lead, width):
    zero = jnp.zeros((PAD, LANES), jnp.float32)
    for index in lead:
        ref[(*index, slice(0, PAD))] = zero
        ref[(*index, slice(PAD + width, 2 * PAD + width))] = zero


def strips_body(rows, width, lat_count, face_ref, mine_ref, other_ref, far_first, far_second, strips, weights, last):
    solver = Solver(rows, width, lat_count, face_ref, mine_ref, other_ref, weights)
    middle = slice(PAD, PAD + width)
    clear_pads(strips, [(j, a, s) for j in range(SWEEPS) for a in range(4) for s in range(2)], width)
    for slab, ref in solver.payloads:
        for row in range(rows):
            strips[0, row, slab, middle] = ref[row * width : (row + 1) * width]
    source = lambda row, slab: jnp.where(
        (solver.core == 0) == (slab == 0),
        mine_ref[(rows + row) * width : (rows + row + 1) * width],
        other_ref[(rows + row) * width : (rows + row + 1) * width],
    )
    top = rows - 1
    for reach in range(1, SWEEPS + 1):
        old = functools.partial(lambda at, a, s, cut: strips[at, a, s, cut], reach - 1)

        def sums(k, slab):
            if k in (0, 3):
                return old(0 if k == 0 else top, slab, middle)
            inner, edge = (1, 0) if k == 1 else (top - 1, top)
            return (
                old(inner, slab, middle)
                + old(edge, slab, slice(PAD - 1, PAD - 1 + width))
                + old(edge, slab, slice(PAD + 1, PAD + 1 + width))
            )

        def unders(k):
            return None if k in (0, 3) else old(0 if k == 1 else top, 1, middle)

        def extras(k, slab):
            return source(0 if k == 1 else top, slab) if reach == 1 and k in (1, 2) else None

        def store(k, slab, value):
            if reach < SWEEPS:
                strips[reach, k, slab, middle] = value
            else:
                last[k, slab] = value

        at = [SWEEPS - reach, SWEEPS + 1 - reach, SWEEPS + top - 1 + reach, SWEEPS + top + reach]
        for group in [(0,), (3,), (1,), (2,)]:
            solver.advance(
                [at[k] for k in group],
                lambda k, slab, group=group: sums(group[k], slab),
                lambda k, group=group: unders(group[k]),
                lambda k, slab, group=group: extras(group[k], slab),
                lambda k, slab, value, group=group: store(group[k], slab, value),
            )
    start = pl.multiple_of(OVERLAP * solver.core, 8)
    half = width - OVERLAP
    odd = solver.odd
    for ref, row in ((far_first, 2 - 2 * odd), (far_second, 2 * odd)):
        for k in range(2):
            for slab in range(2):
                ref[k, slab] = last[row + k, slab, pl.ds(start, half)]


def sums_of(solver, old, at):
    rows, width = solver.rows, solver.width
    middle = slice(PAD, PAD + width)

    def beside(row, step, slab):
        value = old(row + step, slab, middle)
        edges = {-1: (SWEEPS - rows, SWEEPS), 1: (SWEEPS + rows - 1, SWEEPS + 2 * rows - 1)}[step]
        return value * solver.inside(row + step) if row in edges else value

    def sums(k, slab):
        row = at[k]
        return (beside(row, -1, slab) + beside(row, 1, slab)) + (
            old(row, slab, slice(PAD - 1, PAD - 1 + width)) + old(row, slab, slice(PAD + 1, PAD + 1 + width))
        )

    return sums


def middle_body(rows, width, lat_count, face_ref, mine_ref, other_ref, strips,
                mid_first, mid_second, inner, source_ref, weights, last):
    solver = Solver(rows, width, lat_count, face_ref, mine_ref, other_ref, weights)
    middle = slice(PAD, PAD + width)
    clear_pads(inner, [(j, a, s) for j in range(SWEEPS - 1) for a in range(4) for s in range(2)], width)
    for slab, ref in solver.payloads:
        for row in range(rows):
            source_ref[slab, row] = ref[(rows + row) * width : (rows + row + 1) * width]

    def sweep(reach):
        low, high = SWEEPS + 2 - reach, SWEEPS + rows - 4 + reach
        at = [low, low + 1] if reach == 1 else [low, low + 1, high, high + 1]

        def old(row, slab, cut):
            for index, first in ((0, low - 1), (2, high + 1)):
                if row - first in (0, 1):
                    return strips[reach - 1, index + row - first, slab, cut]
            for index, first in ((0, low + 1), (2, high - 1)):
                if row - first in (0, 1):
                    return inner[reach - 2, index + row - first, slab, cut]
            raise ValueError(row)

        def store(k, slab, value):
            if reach == SWEEPS:
                last[k, slab] = value
                return
            inner[reach - 1, k, slab, middle] = value
            if reach == 1:
                inner[reach - 1, 2 + k, slab, middle] = value

        def extras(k, slab):
            return source_ref[slab, at[k] - SWEEPS] if 0 <= at[k] - SWEEPS < rows else None

        solver.advance(at, sums_of(solver, old, at), lambda k: old(at[k], 1, middle), extras, store)

    for reach in range(1, SWEEPS + 1):
        sweep(reach)
    start = pl.multiple_of(OVERLAP * solver.core, 8)
    half = width - OVERLAP
    odd = solver.odd
    for ref, row in ((mid_first, 2 - 2 * odd), (mid_second, 2 * odd)):
        for k in range(2):
            for slab in range(2):
                ref[k, slab] = last[row + k, slab, pl.ds(start, half)]


def core_body(rows, width, lat_count, face_ref, mine_ref, other_ref, inner, source_ref,
              near_first, near_second, own, field, weights):
    solver = Solver(rows, width, lat_count, face_ref, mine_ref, other_ref, weights)
    middle = slice(PAD, PAD + width)
    half = width - OVERLAP
    clear_pads(field, [(b, s, r) for b in range(2) for s in range(2) for r in range(field.shape[2])], width)

    def sweep(reach):
        low, high = SWEEPS + 3 - reach, SWEEPS + rows - 5 + reach

        def old(row, slab, cut):
            for index, first in ((0, low), (2, high)):
                if row - first in (0, 1):
                    return inner[reach - 2, index + row - first, slab, cut]
            return field[(reach + 1) % 2, slab, row - 4, cut]

        def group(at):
            def store(k, slab, value):
                field[reach % 2, slab, at[k] - 4, middle] = value

            def extras(k, slab):
                return source_ref[slab, at[k] - SWEEPS] if 0 <= at[k] - SWEEPS < rows else None

            solver.advance(at, sums_of(solver, old, at), lambda k: old(at[k], 1, middle), extras, store)

        todo = list(range(low + 1, high + 1))
        for first in range(0, len(todo), GROUP):
            group(todo[first : first + GROUP])

    for reach in range(3, SWEEPS + 1):
        sweep(reach)
    start = pl.multiple_of(PAD + OVERLAP * solver.core, 8)
    odd = solver.odd
    for ref, row in ((own, 2), (near_first, 6 - 6 * odd), (near_second, 6 * odd)):
        for k in range(ref.shape[0]):
            for slab in range(2):
                ref[k, slab] = field[SWEEPS % 2, slab, row + k, pl.ds(start, half)]


def sweeps(face, mine, other, rows, half, lat_count):
    width = half + OVERLAP
    shape = lambda count: jax.ShapeDtypeStruct((count, 2, half, LANES), jnp.float32)
    weights = pltpu.VMEM((2, 2 * LANES, 2 * LANES), jnp.bfloat16)
    far_first, far_second, strips = pl.pallas_call(
        functools.partial(strips_body, rows, width, lat_count),
        out_shape=[
            shape(2),
            shape(2),
            jax.ShapeDtypeStruct((SWEEPS, 4, 2, width + 2 * PAD, LANES), jnp.float32),
        ],
        in_specs=[SMEM] + [VMEM] * 2,
        out_specs=[VMEM] * 3,
        scratch_shapes=[weights, pltpu.VMEM((4, 2, width, LANES), jnp.float32)],
        compiler_params=pltpu.CompilerParams(vmem_limit_bytes=24 * 2**20),
        name="strips",
    )(face, mine, other)
    mid_first, mid_second, inner, terms = pl.pallas_call(
        functools.partial(middle_body, rows, width, lat_count),
        out_shape=[
            shape(2),
            shape(2),
            jax.ShapeDtypeStruct((SWEEPS - 1, 4, 2, width + 2 * PAD, LANES), jnp.float32),
            jax.ShapeDtypeStruct((2, rows, width, LANES), jnp.float32),
        ],
        in_specs=[SMEM] + [VMEM] * 3,
        out_specs=[VMEM] * 4,
        scratch_shapes=[weights, pltpu.VMEM((4, 2, width, LANES), jnp.float32)],
        compiler_params=pltpu.CompilerParams(vmem_limit_bytes=32 * 2**20),
        name="middle",
    )(face, mine, other, strips)
    near_first, near_second, own = pl.pallas_call(
        functools.partial(core_body, rows, width, lat_count),
        out_shape=[shape(k) for k in (2, 2, rows)],
        in_specs=[SMEM] + [VMEM] * 4,
        out_specs=[VMEM] * 3,
        scratch_shapes=[pltpu.VMEM((2, 2, rows + 4, width + 2 * PAD, LANES), jnp.float32), weights],
        compiler_params=pltpu.CompilerParams(vmem_limit_bytes=32 * 2**20),
        name="core",
    )(face, mine, other, inner, terms)
    return far_first, far_second, mid_first, mid_second, near_first, near_second, own


def join_body(near, far, same, cross):
    core, _ = position()
    for k in range(near.shape[0]):
        same[k] = near[k, core] + far[k, core]
        cross[k] = near[k, 1 - core] + far[k, 1 - core]


def hand_body(own, mid_first, mid_second, kept, handed):
    core, lat = position()
    odd = lax.rem(lat, 2)
    for piece, pair in ((mid_first, odd), (mid_second, 1 - odd)):
        for k in range(2):
            row = 2 * pair + k
            kept[row] = own[row, core] + piece[k, core]
            handed[row] = own[row, 1 - core] + piece[k, 1 - core]


def finish_body(crossed, parts, base, *refs):
    pieces = dict(zip(parts, refs))
    out_hbm, lines, sems = refs[-3:]
    at_core, lat = position()
    rows, half, _ = base.shape
    tiles = half // LANES
    step = 2 * tiles * rows
    for core in range(2):
        for odd in range(2):

            @pl.when((at_core == core) & (lax.rem(lat, 2) == odd))
            def _():
                side = 1 - core if crossed else core
                copies = []
                for tile in range(tiles):
                    cut = slice(tile * LANES, (tile + 1) * LANES)
                    todo = [row for row in range(rows) if (row // 2 == odd) in parts]
                    for row in todo:
                        value = base[row, cut] + pieces[row // 2 == odd][row % 2, cut]
                        line = core * tiles * rows + tile * rows + row
                        lines[pl.ds(line, LANES, stride=tiles * rows), :] = value.T
                    at, count = tile * rows + todo[0], len(todo)
                    if core == 1:
                        last = LANES * tiles * rows + at
                        lines[at : at + count] = lines[last : last + count]
                    copies.append(
                        pltpu.make_async_copy(
                            lines.reshape(LANES + 1, tiles * rows, LANES).at[pl.ds(0, LANES), pl.ds(at, count)],
                            out_hbm.reshape(LANES, step, LANES).at[:, pl.ds(side * tiles * rows + at, count)],
                            sems.at[tile],
                        )
                    )
                    copies[-1].start()
                for copy in copies:
                    copy.wait()


def finish(base, pieces, lines, before=None):
    _, half, _ = base.shape
    hbm = pl.BlockSpec(memory_space=pltpu.HBM)
    crossed = before is not None
    return pl.pallas_call(
        functools.partial(finish_body, crossed, tuple(pieces)),
        out_shape=jax.ShapeDtypeStruct((lines, LANES), jnp.float32),
        in_specs=[VMEM] * (1 + len(pieces)) + [hbm] * crossed,
        out_specs=hbm,
        scratch_shapes=[
            pltpu.VMEM((lines // LANES * (LANES + 1) // 2, LANES), jnp.float32),
            pltpu.SemaphoreType.DMA((half // LANES,)),
        ],
        input_output_aliases={1 + len(pieces): 0} if crossed else {},
        compiler_params=pltpu.CompilerParams(vmem_limit_bytes=8 * 2**20),
    )(base, *pieces.values(), *([before] if crossed else []))


def program(temp_old, source, lat_couple, face_couple, block_inverse):
    _, rows, columns = temp_old.shape
    half = columns // 2
    lat_count = lax.axis_size("lat")
    params = pltpu.CompilerParams(vmem_limit_bytes=16 * 2**20)
    piece = lambda *shape: jax.ShapeDtypeStruct((*shape, half, LANES), jnp.float32)

    def call(body, outs, *arrays):
        return pl.pallas_call(
            body, out_shape=outs, in_specs=[VMEM] * len(arrays), out_specs=[VMEM] * len(outs),
            compiler_params=params,
        )(*arrays)

    pairs = [
        [(i, i + 1) for i in range(start, lat_count - 1, 2)] + [(i + 1, i) for i in range(start, lat_count - 1, 2)]
        for start in (0, 1)
    ]
    last = lat_count - 1
    far_pairs = [[pair for pair in group if pair not in ((1, 0), (last - 1, last))] for group in pairs]
    crossed = [
        [(d * lat_count + a, (1 - d) * lat_count + b) for d in range(2) for a, b in group] for group in pairs
    ]

    swap = lambda value: lax.ppermute(value, "depth", [(0, 1), (1, 0)])
    exchange = lambda value, group: lax.ppermute(value, "lat", pairs[group])
    cross = lambda value, group: lax.ppermute(value, ("depth", "lat"), crossed[group])

    temp, src = lines_of(temp_old), lines_of(source)
    sent, *held = pack_send(rows, temp, src, block_inverse, lat_couple.reshape(1, LANES))
    other = swap(sent)
    mine = pack_own(rows, temp, src, *held, sent)
    far_first, far_second, mid_first, mid_second, near_first, near_second, own = sweeps(
        face_couple, mine, other, rows, half, lat_count
    )
    far_first, far_second = (
        lax.ppermute(value, "lat", far_pairs[group]) for group, value in enumerate((far_first, far_second))
    )
    mid_first, mid_second = exchange(mid_first, 0), exchange(mid_second, 1)
    joined = [piece(2), piece(2)]
    same_second, cross_second = call(join_body, joined, near_second, far_first)
    same_second, cross_second = exchange(same_second, 1), cross(cross_second, 1)
    same_first, cross_first = call(join_body, joined, near_first, far_second)
    same_first, cross_first = exchange(same_first, 0), cross(cross_first, 0)
    kept, handed = call(hand_body, [piece(rows), piece(rows)], own, mid_first, mid_second)
    lines = temp_old.size // LANES
    result = finish(kept, {False: same_first, True: same_second}, lines)
    handed = swap(handed)
    for pieces in FINISH:
        crossed = {False: cross_first, True: cross_second}
        result = finish(handed, {part: crossed[part] for part in pieces}, lines, result)
    return array_of(result, temp_old.shape)


def solution(mesh):
    return jax.shard_map(
        program,
        mesh=mesh,
        in_specs=(
            P("depth", "lat", None),
            P("depth", "lat", None),
            P("depth"),
            P(),
            P("depth", None),
        ),
        out_specs=P("depth", "lat", None),
        check_vma=False,
    )
```

```python
import functools
import jax
import jax.numpy as jnp
from jax import lax
from jax.experimental import pallas as pl
from jax.experimental.pallas import tpu as pltpu
from jax.sharding import PartitionSpec as P


SWEEPS = 6
LANES = 128
OVERLAP = 16
PAD = 8
GROUP = 2
FINISH = ((True,), (False,))
VMEM = pl.BlockSpec(memory_space=pltpu.VMEM)
SMEM = pl.BlockSpec(memory_space=pltpu.SMEM)


def position():
    return lax.axis_index("depth"), lax.axis_index("lat")


def lines_of(array):
    layers, rows, columns = array.shape
    return array.reshape(layers, rows, columns // LANES, LANES).transpose(0, 2, 1, 3).reshape(-1, LANES)


def array_of(lines, shape):
    layers, rows, columns = shape
    return lines.reshape(layers, columns // LANES, rows, LANES).transpose(0, 2, 1, 3).reshape(shape)


def window_pieces(rows, step, upper):
    tiles = step // rows // 2
    half = tiles * LANES
    if not upper:
        return [(t, 0, LANES, t * LANES) for t in range(tiles)] + [(tiles, 0, OVERLAP, half)]
    return [(tiles + t, 0, LANES, OVERLAP + t * LANES) for t in range(tiles)] + [
        (tiles - 1, LANES - OVERLAP, OVERLAP, 0)
    ]


def pack_piece(rows, slab, ref, array, piece, out_ref, scale=None):
    step = ref.shape[0] // (LANES + 1)
    width = step // rows // 2 * LANES + OVERLAP
    tile, first, count, place = piece
    for row in range(rows):
        base = (array * rows + row) * width + place
        block = ref[pl.ds((slab * step) + tile * rows + row, LANES, stride=step), :].T
        block = block[first : first + count]
        out_ref[base : base + count, :] = block if scale is None else block * scale


def tile_copy(rows, hbm, ref, tile, sem):
    target = ref.reshape(LANES + 1, ref.shape[0] // (LANES + 1), LANES)
    cut = pl.ds(tile * rows, rows)
    return pltpu.make_async_copy(
        hbm.reshape(LANES, hbm.shape[0] // LANES, LANES).at[:, cut], target.at[pl.ds(0, LANES), cut], sem
    )


def repeat_first(rows, ref, tile):
    last = ref.shape[0] - ref.shape[0] // (LANES + 1) + tile * rows
    ref[last : last + rows] = ref[tile * rows : (tile + 1) * rows]


def pack_send_body(rows, temp_hbm, source_hbm, inverse_hbm, couple_hbm,
                   out_ref, temp_ref, source_ref, inverse_ref, couple_ref, sems):
    at_core, _ = position()
    step = temp_hbm.shape[0] // LANES
    tiles = step // rows
    arrays = ((temp_hbm, temp_ref), (source_hbm, source_ref))

    def array_copy(array, tile):
        return tile_copy(rows, *arrays[array], tile, sems.at[array * tiles + tile])

    inverse_copy = pltpu.make_async_copy(inverse_hbm, inverse_ref, sems.at[2 * tiles])
    couple_copy = pltpu.make_async_copy(couple_hbm, couple_ref, sems.at[2 * tiles + 1])
    for slab in range(2):
        pieces = window_pieces(rows, step, slab == 0)
        turned = (lambda value: pltpu.roll(value, LANES - 1, 1)) if slab == 1 else (lambda value: value)

        @pl.when(at_core == slab)
        def _():
            inverse_copy.start()
            couple_copy.start()
            for array in range(2):
                for piece in pieces:
                    array_copy(array, piece[0]).start()

            def arrive(array, tile):
                array_copy(array, tile).wait()
                if slab == 1:
                    repeat_first(rows, arrays[array][1], tile)

            inverse_copy.wait()
            couple_copy.wait()
            base = out_ref.shape[0] - LANES - 8
            inverse = turned((inverse_ref[...] * couple_ref[...]).T)
            if slab == 1:
                inverse = pltpu.roll(inverse, LANES - 1, 0)
            out_ref[base : base + LANES, :] = inverse
            scale = 1.0 / turned(jnp.broadcast_to(couple_ref[...], (8, LANES)))
            out_ref[base + LANES :, :] = scale
            for array in range(2):
                for piece in pieces:
                    arrive(array, piece[0])
                    pack_piece(
                        rows, slab, arrays[array][1], array, piece, out_ref, scale[0:1] if array == 1 else None
                    )


def pack_own_body(rows, temp_hbm, source_hbm, temp_ref, source_ref, sent_ref, out_ref, more_temp, more_source, sems):
    core, _ = position()
    step = temp_hbm.shape[0] // LANES
    arrays = ((temp_hbm, temp_ref, more_temp), (source_hbm, source_ref, more_source))
    base = out_ref.shape[0] - LANES - 8
    scale = (None, sent_ref[base + LANES : base + LANES + 1, :])
    for slab in range(2):

        @pl.when(core == slab)
        def _():
            held = [piece[0] for piece in window_pieces(rows, step, slab == 0)]
            pieces = window_pieces(rows, step, slab == 1)
            (tile,) = [at for at in range(step // rows) if at not in held]
            copies = [tile_copy(rows, hbm, more, tile, sems.at[at]) for at, (hbm, _, more) in enumerate(arrays)]
            for copy in copies:
                copy.start()
            for array, (_, ref, _) in enumerate(arrays):
                for piece in pieces:
                    if piece[0] != tile:
                        pack_piece(rows, slab, ref, array, piece, out_ref, scale[array])
            for array, (_, _, more) in enumerate(arrays):
                copies[array].wait()
                if slab == 1:
                    repeat_first(rows, more, tile)
                for piece in pieces:
                    if piece[0] == tile:
                        pack_piece(rows, slab, more, array, piece, out_ref, scale[array])

    out_ref[base:, :] = sent_ref[base:, :]


def pack_own(rows, temp, source, temp_held, source_held, sent):
    hbm = pl.BlockSpec(memory_space=pltpu.HBM)
    lines = pltpu.VMEM(temp_held.shape, jnp.float32)
    return pl.pallas_call(
        functools.partial(pack_own_body, rows),
        out_shape=jax.ShapeDtypeStruct(sent.shape, jnp.float32),
        in_specs=[hbm] * 2 + [VMEM] * 3,
        out_specs=VMEM,
        scratch_shapes=[lines, lines, pltpu.SemaphoreType.DMA((2,))],
        compiler_params=pltpu.CompilerParams(vmem_limit_bytes=12 * 2**20),
        name="pack_own",
    )(*(pltpu.with_memory_space_constraint(array, pltpu.HBM) for array in (temp, source)), temp_held, source_held, sent)


def pack_send(rows, temp, source, inverse, couple):
    columns = temp.shape[0] // rows
    length = 2 * rows * (columns // 2 + OVERLAP) + LANES + 8
    shape = lambda count: jax.ShapeDtypeStruct((count, LANES), jnp.float32)
    lines = shape(temp.shape[0] // LANES * (LANES + 1))
    return pl.pallas_call(
        functools.partial(pack_send_body, rows),
        out_shape=[shape(length), lines, lines],
        in_specs=[pl.BlockSpec(memory_space=pltpu.HBM)] * 4,
        out_specs=[VMEM] * 3,
        scratch_shapes=[
            pltpu.VMEM(inverse.shape, jnp.float32),
            pltpu.VMEM(couple.shape, jnp.float32),
            pltpu.SemaphoreType.DMA((2 * columns // LANES + 2,)),
        ],
        compiler_params=pltpu.CompilerParams(vmem_limit_bytes=12 * 2**20),
        name="pack_send",
    )(*(pltpu.with_memory_space_constraint(array, pltpu.HBM) for array in (temp, source, inverse, couple)))


def split(value):
    high = value.astype(jnp.bfloat16)
    return high, (value - high.astype(jnp.float32)).astype(jnp.bfloat16)


class Solver:
    def __init__(self, rows, width, lat_count, face_ref, mine_ref, other_ref, weights):
        self.rows, self.width, self.weights, self.lat_count = rows, width, weights, lat_count
        self.core, self.lat = position()
        self.odd = lax.rem(self.lat, 2)
        self.payloads = ((self.core, mine_ref), (1 - self.core, other_ref))
        base = 2 * rows * width
        first = self.core == 0
        face = face_ref[0]

        def pick(start, count, slab):
            return jnp.where(first == (slab == 0), mine_ref[start : start + count], other_ref[start : start + count])

        for slab in range(2):
            high, low = split(pick(base, LANES, slab))
            weights[slab, :LANES, :LANES] = high
            weights[slab, LANES:, :LANES] = high
            weights[slab, :LANES, LANES:] = low
            weights[slab, LANES:, LANES:] = jnp.zeros((LANES, LANES), jnp.bfloat16)
        lane = lax.broadcasted_iota(jnp.int32, (1, LANES), 1)
        self.face_last = [
            jnp.where(lane == LANES - 1, face * pick(base + LANES, 8, slab)[0:1], 0.0) for slab in range(2)
        ]

    def inside(self, row):
        grid_row = self.lat * self.rows - SWEEPS + row
        return ((grid_row >= 0) & (grid_row < self.lat_count * self.rows)).astype(jnp.float32)

    def apply(self, slab, sides):
        high, low = split(jnp.concatenate(sides, axis=0))
        both = jnp.dot(
            jnp.concatenate([high, low], axis=1), self.weights[slab], preferred_element_type=jnp.float32
        )
        solved = both[:, :LANES] + both[:, LANES:]
        return [solved[k * self.width : (k + 1) * self.width] for k in range(len(sides))]

    def advance(self, rows, sums, unders, extras, store):
        def side(k, slab):
            value = sums(k, slab)
            extra = extras(k, slab)
            return value if extra is None else value + extra

        upper = []
        for k in range(len(rows)):
            value, under = side(k, 0), unders(k)
            upper.append(value if under is None else value + under * self.face_last[0])
        upper = self.apply(0, upper)
        for k, value in enumerate(upper):
            store(k, 0, value)
        lower = self.apply(
            1, [side(k, 1) + upper[k] * self.face_last[1] for k in range(len(rows))]
        )
        for k, value in enumerate(lower):
            store(k, 1, value)


def clear_pads(ref, lead, width):
    zero = jnp.zeros((PAD, LANES), jnp.float32)
    for index in lead:
        ref[(*index, slice(0, PAD))] = zero
        ref[(*index, slice(PAD + width, 2 * PAD + width))] = zero


def strips_body(rows, width, lat_count, face_ref, mine_ref, other_ref, far_first, far_second, strips, weights, last):
    solver = Solver(rows, width, lat_count, face_ref, mine_ref, other_ref, weights)
    middle = slice(PAD, PAD + width)
    clear_pads(strips, [(j, a, s) for j in range(SWEEPS) for a in range(4) for s in range(2)], width)
    for slab, ref in solver.payloads:
        for row in range(rows):
            strips[0, row, slab, middle] = ref[row * width : (row + 1) * width]
    source = lambda row, slab: jnp.where(
        (solver.core == 0) == (slab == 0),
        mine_ref[(rows + row) * width : (rows + row + 1) * width],
        other_ref[(rows + row) * width : (rows + row + 1) * width],
    )
    top = rows - 1
    for reach in range(1, SWEEPS + 1):
        old = functools.partial(lambda at, a, s, cut: strips[at, a, s, cut], reach - 1)

        def sums(k, slab):
            if k in (0, 3):
                return old(0 if k == 0 else top, slab, middle)
            inner, edge = (1, 0) if k == 1 else (top - 1, top)
            return (
                old(inner, slab, middle)
                + old(edge, slab, slice(PAD - 1, PAD - 1 + width))
                + old(edge, slab, slice(PAD + 1, PAD + 1 + width))
            )

        def unders(k):
            return None if k in (0, 3) else old(0 if k == 1 else top, 1, middle)

        def extras(k, slab):
            return source(0 if k == 1 else top, slab) if reach == 1 and k in (1, 2) else None

        def store(k, slab, value):
            if reach < SWEEPS:
                strips[reach, k, slab, middle] = value
            else:
                last[k, slab] = value

        at = [SWEEPS - reach, SWEEPS + 1 - reach, SWEEPS + top - 1 + reach, SWEEPS + top + reach]
        for group in [(0,), (3,), (1,), (2,)]:
            solver.advance(
                [at[k] for k in group],
                lambda k, slab, group=group: sums(group[k], slab),
                lambda k, group=group: unders(group[k]),
                lambda k, slab, group=group: extras(group[k], slab),
                lambda k, slab, value, group=group: store(group[k], slab, value),
            )
    start = pl.multiple_of(OVERLAP * solver.core, 8)
    half = width - OVERLAP
    odd = solver.odd
    for ref, row in ((far_first, 2 - 2 * odd), (far_second, 2 * odd)):
        for k in range(2):
            for slab in range(2):
                ref[k, slab] = last[row + k, slab, pl.ds(start, half)]


def sums_of(solver, old, at):
    rows, width = solver.rows, solver.width
    middle = slice(PAD, PAD + width)

    def beside(row, step, slab):
        value = old(row + step, slab, middle)
        edges = {-1: (SWEEPS - rows, SWEEPS), 1: (SWEEPS + rows - 1, SWEEPS + 2 * rows - 1)}[step]
        return value * solver.inside(row + step) if row in edges else value

    def sums(k, slab):
        row = at[k]
        return (beside(row, -1, slab) + beside(row, 1, slab)) + (
            old(row, slab, slice(PAD - 1, PAD - 1 + width)) + old(row, slab, slice(PAD + 1, PAD + 1 + width))
        )

    return sums


def middle_body(rows, width, lat_count, face_ref, mine_ref, other_ref, strips,
                mid_first, mid_second, inner, source_ref, weights, last):
    solver = Solver(rows, width, lat_count, face_ref, mine_ref, other_ref, weights)
    middle = slice(PAD, PAD + width)
    clear_pads(inner, [(j, a, s) for j in range(SWEEPS - 1) for a in range(4) for s in range(2)], width)
    for slab, ref in solver.payloads:
        for row in range(rows):
            source_ref[slab, row] = ref[(rows + row) * width : (rows + row + 1) * width]

    def sweep(reach):
        low, high = SWEEPS + 2 - reach, SWEEPS + rows - 4 + reach
        at = [low, low + 1] if reach == 1 else [low, low + 1, high, high + 1]

        def old(row, slab, cut):
            for index, first in ((0, low - 1), (2, high + 1)):
                if row - first in (0, 1):
                    return strips[reach - 1, index + row - first, slab, cut]
            for index, first in ((0, low + 1), (2, high - 1)):
                if row - first in (0, 1):
                    return inner[reach - 2, index + row - first, slab, cut]
            raise ValueError(row)

        def store(k, slab, value):
            if reach == SWEEPS:
                last[k, slab] = value
                return
            inner[reach - 1, k, slab, middle] = value
            if reach == 1:
                inner[reach - 1, 2 + k, slab, middle] = value

        def extras(k, slab):
            return source_ref[slab, at[k] - SWEEPS] if 0 <= at[k] - SWEEPS < rows else None

        solver.advance(at, sums_of(solver, old, at), lambda k: old(at[k], 1, middle), extras, store)

    for reach in range(1, SWEEPS + 1):
        sweep(reach)
    start = pl.multiple_of(OVERLAP * solver.core, 8)
    half = width - OVERLAP
    odd = solver.odd
    for ref, row in ((mid_first, 2 - 2 * odd), (mid_second, 2 * odd)):
        for k in range(2):
            for slab in range(2):
                ref[k, slab] = last[row + k, slab, pl.ds(start, half)]


def core_body(rows, width, lat_count, face_ref, mine_ref, other_ref, inner, source_ref,
              near_first, near_second, own, field, weights):
    solver = Solver(rows, width, lat_count, face_ref, mine_ref, other_ref, weights)
    middle = slice(PAD, PAD + width)
    half = width - OVERLAP
    clear_pads(field, [(b, s, r) for b in range(2) for s in range(2) for r in range(field.shape[2])], width)

    def sweep(reach):
        low, high = SWEEPS + 3 - reach, SWEEPS + rows - 5 + reach

        def old(row, slab, cut):
            for index, first in ((0, low), (2, high)):
                if row - first in (0, 1):
                    return inner[reach - 2, index + row - first, slab, cut]
            return field[(reach + 1) % 2, slab, row - 4, cut]

        def group(at):
            def store(k, slab, value):
                field[reach % 2, slab, at[k] - 4, middle] = value

            def extras(k, slab):
                return source_ref[slab, at[k] - SWEEPS] if 0 <= at[k] - SWEEPS < rows else None

            solver.advance(at, sums_of(solver, old, at), lambda k: old(at[k], 1, middle), extras, store)

        todo = list(range(low + 1, high + 1))
        for first in range(0, len(todo), GROUP):
            group(todo[first : first + GROUP])

    for reach in range(3, SWEEPS + 1):
        sweep(reach)
    start = pl.multiple_of(PAD + OVERLAP * solver.core, 8)
    odd = solver.odd
    for ref, row in ((own, 2), (near_first, 6 - 6 * odd), (near_second, 6 * odd)):
        for k in range(ref.shape[0]):
            for slab in range(2):
                ref[k, slab] = field[SWEEPS % 2, slab, row + k, pl.ds(start, half)]


def sweeps(face, mine, other, rows, half, lat_count):
    width = half + OVERLAP
    shape = lambda count: jax.ShapeDtypeStruct((count, 2, half, LANES), jnp.float32)
    weights = pltpu.VMEM((2, 2 * LANES, 2 * LANES), jnp.bfloat16)
    far_first, far_second, strips = pl.pallas_call(
        functools.partial(strips_body, rows, width, lat_count),
        out_shape=[
            shape(2),
            shape(2),
            jax.ShapeDtypeStruct((SWEEPS, 4, 2, width + 2 * PAD, LANES), jnp.float32),
        ],
        in_specs=[SMEM] + [VMEM] * 2,
        out_specs=[VMEM] * 3,
        scratch_shapes=[weights, pltpu.VMEM((4, 2, width, LANES), jnp.float32)],
        compiler_params=pltpu.CompilerParams(vmem_limit_bytes=24 * 2**20),
        name="strips",
    )(face, mine, other)
    mid_first, mid_second, inner, terms = pl.pallas_call(
        functools.partial(middle_body, rows, width, lat_count),
        out_shape=[
            shape(2),
            shape(2),
            jax.ShapeDtypeStruct((SWEEPS - 1, 4, 2, width + 2 * PAD, LANES), jnp.float32),
            jax.ShapeDtypeStruct((2, rows, width, LANES), jnp.float32),
        ],
        in_specs=[SMEM] + [VMEM] * 3,
        out_specs=[VMEM] * 4,
        scratch_shapes=[weights, pltpu.VMEM((4, 2, width, LANES), jnp.float32)],
        compiler_params=pltpu.CompilerParams(vmem_limit_bytes=32 * 2**20),
        name="middle",
    )(face, mine, other, strips)
    near_first, near_second, own = pl.pallas_call(
        functools.partial(core_body, rows, width, lat_count),
        out_shape=[shape(k) for k in (2, 2, rows)],
        in_specs=[SMEM] + [VMEM] * 4,
        out_specs=[VMEM] * 3,
        scratch_shapes=[pltpu.VMEM((2, 2, rows + 4, width + 2 * PAD, LANES), jnp.float32), weights],
        compiler_params=pltpu.CompilerParams(vmem_limit_bytes=32 * 2**20),
        name="core",
    )(face, mine, other, inner, terms)
    return far_first, far_second, mid_first, mid_second, near_first, near_second, own


def join_body(near, far, same, cross):
    core, _ = position()
    for k in range(near.shape[0]):
        same[k] = near[k, core] + far[k, core]
        cross[k] = near[k, 1 - core] + far[k, 1 - core]


def hand_body(own, mid_first, mid_second, kept, handed):
    core, lat = position()
    odd = lax.rem(lat, 2)
    for piece, pair in ((mid_first, odd), (mid_second, 1 - odd)):
        for k in range(2):
            row = 2 * pair + k
            kept[row] = own[row, core] + piece[k, core]
            handed[row] = own[row, 1 - core] + piece[k, 1 - core]


def finish_body(crossed, parts, base, *refs):
    pieces = dict(zip(parts, refs))
    out_hbm, lines, sems = refs[-3:]
    at_core, lat = position()
    rows, half, _ = base.shape
    tiles = half // LANES
    step = 2 * tiles * rows
    for core in range(2):
        for odd in range(2):

            @pl.when((at_core == core) & (lax.rem(lat, 2) == odd))
            def _():
                side = 1 - core if crossed else core
                copies = []
                for tile in range(tiles):
                    cut = slice(tile * LANES, (tile + 1) * LANES)
                    todo = [row for row in range(rows) if (row // 2 == odd) in parts]
                    for row in todo:
                        value = base[row, cut] + pieces[row // 2 == odd][row % 2, cut]
                        line = core * tiles * rows + tile * rows + row
                        lines[pl.ds(line, LANES, stride=tiles * rows), :] = value.T
                    at, count = tile * rows + todo[0], len(todo)
                    if core == 1:
                        last = LANES * tiles * rows + at
                        lines[at : at + count] = lines[last : last + count]
                    copies.append(
                        pltpu.make_async_copy(
                            lines.reshape(LANES + 1, tiles * rows, LANES).at[pl.ds(0, LANES), pl.ds(at, count)],
                            out_hbm.reshape(LANES, step, LANES).at[:, pl.ds(side * tiles * rows + at, count)],
                            sems.at[tile],
                        )
                    )
                    copies[-1].start()
                for copy in copies:
                    copy.wait()


def finish(base, pieces, lines, before=None):
    _, half, _ = base.shape
    hbm = pl.BlockSpec(memory_space=pltpu.HBM)
    crossed = before is not None
    return pl.pallas_call(
        functools.partial(finish_body, crossed, tuple(pieces)),
        out_shape=jax.ShapeDtypeStruct((lines, LANES), jnp.float32),
        in_specs=[VMEM] * (1 + len(pieces)) + [hbm] * crossed,
        out_specs=hbm,
        scratch_shapes=[
            pltpu.VMEM((lines // LANES * (LANES + 1) // 2, LANES), jnp.float32),
            pltpu.SemaphoreType.DMA((half // LANES,)),
        ],
        input_output_aliases={1 + len(pieces): 0} if crossed else {},
        compiler_params=pltpu.CompilerParams(vmem_limit_bytes=8 * 2**20),
    )(base, *pieces.values(), *([before] if crossed else []))


def program(temp_old, source, lat_couple, face_couple, block_inverse):
    _, rows, columns = temp_old.shape
    half = columns // 2
    lat_count = lax.axis_size("lat")
    params = pltpu.CompilerParams(vmem_limit_bytes=16 * 2**20)
    piece = lambda *shape: jax.ShapeDtypeStruct((*shape, half, LANES), jnp.float32)

    def call(body, outs, *arrays):
        return pl.pallas_call(
            body, out_shape=outs, in_specs=[VMEM] * len(arrays), out_specs=[VMEM] * len(outs),
            compiler_params=params,
        )(*arrays)

    pairs = [
        [(i, i + 1) for i in range(start, lat_count - 1, 2)] + [(i + 1, i) for i in range(start, lat_count - 1, 2)]
        for start in (0, 1)
    ]
    crossed = [
        [(d * lat_count + a, (1 - d) * lat_count + b) for d in range(2) for a, b in group] for group in pairs
    ]

    swap = lambda value: lax.ppermute(value, "depth", [(0, 1), (1, 0)])
    exchange = lambda value, group: lax.ppermute(value, "lat", pairs[group])
    cross = lambda value, group: lax.ppermute(value, ("depth", "lat"), crossed[group])

    temp, src = lines_of(temp_old), lines_of(source)
    sent, *held = pack_send(rows, temp, src, block_inverse, lat_couple.reshape(1, LANES))
    other = swap(sent)
    mine = pack_own(rows, temp, src, *held, sent)
    far_first, far_second, mid_first, mid_second, near_first, near_second, own = sweeps(
        face_couple, mine, other, rows, half, lat_count
    )
    far_first, far_second = exchange(far_first, 0), exchange(far_second, 1)
    mid_first, mid_second = exchange(mid_first, 0), exchange(mid_second, 1)
    joined = [piece(2), piece(2)]
    same_second, cross_second = call(join_body, joined, near_second, far_first)
    same_second, cross_second = exchange(same_second, 1), cross(cross_second, 1)
    same_first, cross_first = call(join_body, joined, near_first, far_second)
    same_first, cross_first = exchange(same_first, 0), cross(cross_first, 0)
    kept, handed = call(hand_body, [piece(rows), piece(rows)], own, mid_first, mid_second)
    lines = temp_old.size // LANES
    result = finish(kept, {False: same_first, True: same_second}, lines)
    handed = swap(handed)
    for pieces in FINISH:
        crossed = {False: cross_first, True: cross_second}
        result = finish(handed, {part: crossed[part] for part in pieces}, lines, result)
    return array_of(result, temp_old.shape)


def solution(mesh):
    return jax.shard_map(
        program,
        mesh=mesh,
        in_specs=(
            P("depth", "lat", None),
            P("depth", "lat", None),
            P("depth"),
            P(),
            P("depth", None),
        ),
        out_specs=P("depth", "lat", None),
        check_vma=False,
    )
```
